8 devices in a mesh: batch: 1 (over z), y: 2 (over y), x: 4 (over x, core).
Axes of the slice: x: 2, y: 2, z: 1, core: 2. Of those that a mesh axis runs over, the one named last changes fastest.
Arguments:
- field: float32 [512, 512, 64], P(('batch', 'x'), 'y')
- sub_x: float32 [512, 512], P(('batch', 'x'), 'y')
- diag_x: float32 [512, 512], P(('batch', 'x'), 'y')
- sup_x: float32 [512, 512], P(('batch', 'x'), 'y')
- sub_y: float32 [512, 512], P(('batch', 'x'), 'y')
- diag_y: float32 [512, 512], P(('batch', 'x'), 'y')
- sup_y: float32 [512, 512], P(('batch', 'x'), 'y')
Outputs:
- output: float32 [512, 512, 64], P(('batch', 'x'), 'y')
All inputs are finite; a program needn't handle non-finite values.
Results may differ from the reference program's by a relative error of at most 0.001.
Values sent between devices are 32-bit elements.
A program may use at most 1 GiB of HBM per device.

```python
import jax
import jax.numpy as jnp
from jax import lax

GRID_X = 512
GRID_Y = 512
FIELDS = 64


def setup_inputs(seed: int = 0, part: int = 0) -> dict:
    base_key = jax.random.fold_in(jax.random.key(seed), part)
    sub_keys = jax.random.split(base_key, 7)
    plane_shape = (GRID_X, GRID_Y)

    def coeff_triple(key_sub, key_sup, key_gap):
        sub_mag = jax.random.uniform(key_sub, plane_shape, jnp.float32, 20.0, 100.0)
        sup_mag = jax.random.uniform(key_sup, plane_shape, jnp.float32, 20.0, 100.0)
        diag_gap = jax.random.uniform(key_gap, plane_shape, jnp.float32, 0.1, 0.6)
        return -sub_mag, sub_mag + sup_mag + diag_gap, -sup_mag

    field = jax.random.normal(sub_keys[0], (GRID_X, GRID_Y, FIELDS), jnp.float32)
    sub_x, diag_x, sup_x = coeff_triple(sub_keys[1], sub_keys[2], sub_keys[3])
    sub_y, diag_y, sup_y = coeff_triple(sub_keys[4], sub_keys[5], sub_keys[6])
    return dict(field=field, sub_x=sub_x, diag_x=diag_x, sup_x=sup_x, sub_y=sub_y, diag_y=diag_y, sup_y=sup_y)


def shift_prev(values, along):
    size = values.shape[along]
    first = jnp.zeros_like(lax.slice_in_dim(values, 0, 1, axis=along))
    return jnp.concatenate([first, lax.slice_in_dim(values, 0, size - 1, axis=along)], axis=along)


def shift_next(values, along):
    size = values.shape[along]
    last = jnp.zeros_like(lax.slice_in_dim(values, 0, 1, axis=along))
    return jnp.concatenate([lax.slice_in_dim(values, 1, size, axis=along), last], axis=along)


def apply_op(sub, diag, sup, values, along):
    return sub[..., None] * shift_prev(values, along) + diag[..., None] * values + sup[..., None] * shift_next(values, along)


def thomas_solve(sub, diag, sup, rhs):
    def forward(carry, row):
        prev_ratio, prev_g = carry
        sub_row, diag_row, sup_row, rhs_row = row
        pivot = 1.0 + diag_row - sub_row * prev_ratio
        ratio = sup_row / pivot
        g_row = (rhs_row - sub_row[..., None] * prev_g) / pivot[..., None]
        return (ratio, g_row), (ratio, g_row)

    start_vals = (jnp.zeros_like(diag[0]), jnp.zeros_like(rhs[0]))
    _, (ratios, g_rows) = lax.scan(forward, start_vals, (sub, diag, sup, rhs))

    def backward(next_val, row):
        ratio, g_row = row
        value = g_row - ratio[..., None] * next_val
        return value, value

    _, solved = lax.scan(backward, jnp.zeros_like(rhs[0]), (ratios, g_rows), reverse=True)
    return solved


def reference(field, sub_x, diag_x, sup_x, sub_y, diag_y, sup_y):
    r_one = field - apply_op(sub_y, diag_y, sup_y, field, 1)
    half = thomas_solve(sub_x, diag_x, sup_x, r_one)
    r_two = half - apply_op(sub_x, diag_x, sup_x, half, 0)
    solved_t = thomas_solve(sub_y.T, diag_y.T, sup_y.T, jnp.swapaxes(r_two, 0, 1))
    return jnp.swapaxes(solved_t, 0, 1)
```

```python
import functools

import jax
import jax.numpy as jnp
from jax import lax
from jax.experimental import pallas as pl
from jax.experimental.pallas import tpu as pltpu
from jax.sharding import PartitionSpec as P

MESH = pl.DeviceIdType.MESH
NI, NF, NJ = 128, 64, 256
L, S = 128, 8
FB = NF // S
JB = NJ // L
CH = 4
CB = FB // CH
CV = CB * JB
HR = 8
f32 = jnp.float32


def bcast(ref, row):
    return jnp.broadcast_to(ref[pl.ds(row, 1), :], (S, L))


def bcast_x(ref, row, jb):
    return jnp.broadcast_to(ref[jb, pl.ds(row, 1), :], (S, L))


def reduce_kernel(u_hbm, sub_x, diag_x, sup_x, sub_y, diag_y, sup_y,
                  g_out, edge_out, ratio_out,
                  b1, b2, b3, halo_send, halo_recv,
                  low_x, cen_x, high_x, inv_x, s_x, p_x, f_x, q_x,
                  cen_t, lo_t, hi_t, b_t, a_t, c_t, inv_t, s_t,
                  coef_send, coef_recv, mu_send, mu_recv,
                  fl_send, fl_recv, lam_send, lam_recv, wprev, wnext,
                  yl_send, yl_recv,
                  in_sem, halo_ss, halo_rs, coef_ss, coef_rs, mu_ss, mu_rs,
                  fl_ss, fl_rs, lam_ss, lam_rs, y_ss, y_rs):
    my_x = lax.axis_index("x")
    my_y = lax.axis_index("y")
    core = lax.rem(my_x, 2)
    chip = my_x // 2
    mate = {"x": my_x + 1 - 2 * core}
    across = {"x": lax.rem(my_x + 2, 4)}
    beside = {"y": 1 - my_y}
    first_core = core == 0
    first_chip = chip == 0
    first_y = my_y == 0

    barrier = pltpu.get_barrier_semaphore()
    for peer in (mate, across, beside):
        pl.semaphore_signal(barrier, inc=1, device_id=peer, device_id_type=MESH)

    def in_copy(fb, jb):
        k = fb * JB + jb
        return pltpu.make_async_copy(
            u_hbm.at[:, pl.ds(fb * S, S), pl.ds(jb * L, L)], b1.at[k], in_sem.at[k])

    for fb in range(FB):
        for jb in range(JB):
            in_copy(fb, jb).start()

    for jb in range(JB):
        cols = slice(jb * L, (jb + 1) * L)
        d = diag_y[:, cols].T
        lo = sub_y[:, cols].T
        hi = sup_y[:, cols].T
        cen_t[cols, :] = 1.0 - d
        b_t[cols, :] = 1.0 + d
        lo_t[cols, :] = lo
        hi_t[cols, :] = hi
        a_t[cols, :] = jnp.where(first_y, lo, hi)
        c_t[cols, :] = jnp.where(first_y, hi, lo)

    for jb in range(JB):
        cols = slice(jb * L, (jb + 1) * L)
        low_x[jb] = sub_x[:, cols]
        cen_x[jb] = 1.0 + diag_x[:, cols]
        high_x[jb] = sup_x[:, cols]

    def x_factor(i, state):
        row = pl.ds(i, 1)
        out = []
        for jb in range(JB):
            p_prev, f_prev, q, e_sum = state[jb]
            sub, sup = low_x[jb, row, :], high_x[jb, row, :]
            inv = 1.0 / (cen_x[jb, row, :] - sub * p_prev)
            p, s = sup * inv, sub * inv
            fill = -s * f_prev
            inv_x[jb, row, :] = inv
            s_x[jb, row, :] = s
            p_x[jb, row, :] = p
            f_x[jb, row, :] = fill
            q_x[jb, row, :] = q
            out.append((p, fill, -q * p, e_sum + q * fill))
        return tuple(out)

    none = jnp.zeros((1, L), f32)
    ends = lax.fori_loop(0, NI, x_factor, ((none, none + 1.0, none + 1.0, none),) * JB)
    for jb in range(JB):
        p_last, f_last, q_all, e_sum = ends[jb]
        for r, value in enumerate((e_sum, f_last, q_all, -p_last)):
            coef_send[jb, r:r + 1, :] = value
        coef_send[jb, 4:8, :] = jnp.zeros((4, L), f32)

    def y_factor(t, p_prev):
        j = jnp.where(first_y, t, NJ - 1 - t)
        row = pl.ds(j, 1)
        low = a_t[row, :]
        inv = 1.0 / (b_t[row, :] - low * p_prev)
        p = c_t[row, :] * inv
        inv_t[row, :] = inv
        s_t[row, :] = low * inv
        ratio_out[row, :] = p
        return p

    p_end = lax.fori_loop(0, NJ, y_factor, jnp.zeros((1, L), f32))

    pl.semaphore_wait(barrier, 3)

    coef_copy = pltpu.make_async_remote_copy(
        coef_send, coef_recv, coef_ss, coef_rs, device_id=mate, device_id_type=MESH)
    coef_copy.start()

    def halo_copy(fb):
        rows = pl.ds(pl.multiple_of(fb * S, S), S)
        return pltpu.make_async_remote_copy(
            halo_send.at[rows, :], halo_recv.at[rows, :], halo_ss.at[fb], halo_rs.at[fb],
            device_id=beside, device_id_type=MESH)

    def to_columns(fb, _):
        for jb in range(JB):
            in_copy(fb, jb).wait()
        views = [b1.at[fb * JB + jb].reshape(NI * S, L) for jb in range(JB)]
        for f in range(S):
            parts = [views[jb][pl.ds(f, NI, stride=S), :].T for jb in range(JB)]
            for jb in range(JB):
                b2[fb * S + f, HR + jb * L:HR + (jb + 1) * L, :] = parts[jb]
            halo_send[pl.ds(fb * S + f, 1), :] = jnp.where(
                first_y, parts[JB - 1][L - 1:L, :], parts[0][0:1, :])
        halo_copy(fb).start()
        return 0

    lax.fori_loop(0, FB, to_columns, 0)

    def stencil(fi, fb):
        f_all = fb * S + fi
        halo = halo_recv[pl.ds(f_all, 1), :]
        none = jnp.zeros_like(halo)
        b2[f_all, HR - 1:HR, :] = jnp.where(first_y, none, halo)
        b2[f_all, HR + NJ:HR + NJ + 1, :] = jnp.where(first_y, halo, none)
        for jb in range(JB):
            base = HR + jb * L
            cols = slice(jb * L, (jb + 1) * L)
            before = b2[f_all, base - 1:base - 1 + L, :]
            here = b2[f_all, base:base + L, :]
            after = b2[f_all, base + 1:base + 1 + L, :]
            r = cen_t[cols, :] * here - lo_t[cols, :] * before - hi_t[cols, :] * after
            b1.at[fb * JB + jb].reshape(NI * S, L)[pl.ds(fi, NI, stride=S), :] = r.T
        return fb

    def fl_copy(c):
        return pltpu.make_async_remote_copy(
            fl_send.at[c], fl_recv.at[c], fl_ss.at[c], fl_rs.at[c], device_id=mate, device_id_type=MESH)

    def lam_copy(c):
        return pltpu.make_async_remote_copy(
            lam_send.at[c], lam_recv.at[c], lam_ss.at[c], lam_rs.at[c], device_id=across, device_id_type=MESH)

    mu_copy = pltpu.make_async_remote_copy(
        mu_send, mu_recv, mu_ss, mu_rs, device_id=across, device_id_type=MESH)

    def x_forward(c):
        def step(i, state):
            gs, accs = state
            inv = [bcast_x(inv_x, i, jb) for jb in range(JB)]
            s = [bcast_x(s_x, i, jb) for jb in range(JB)]
            q = [bcast_x(q_x, i, jb) for jb in range(JB)]
            new_g, new_acc = [], []
            for v in range(CV):
                jb = v % JB
                g = b1[c * CV + v, i] * inv[jb] - s[jb] * gs[v]
                b3[c * CV + v, i] = g
                new_g.append(g)
                new_acc.append(accs[v] + q[jb] * g)
            return tuple(new_g), tuple(new_acc)

        zeros = tuple(jnp.zeros((S, L), f32) for _ in range(CV))
        gs, accs = lax.fori_loop(0, NI, step, (zeros, zeros), unroll=4)
        for v in range(CV):
            fl_send[c, 0, v] = accs[v]
            fl_send[c, 1, v] = gs[v]
        fl_copy(c).start()

    def pair_coefs(jb):
        def both(row):
            mine, other = coef_send[jb, row:row + 1, :], coef_recv[jb, row:row + 1, :]
            return jnp.where(first_core, mine, other), jnp.where(first_core, other, mine)

        ef, el, qf, ql = both(0), both(1), both(2), both(3)
        return ef, el, qf, ql, 1.0 / (1.0 - ql[0] * ef[1])

    def own_mu(jb):
        ef, el, qf, ql, det = pair_coefs(jb)
        return jnp.where(first_chip, el[1] * det * ql[0] * qf[1] + ql[1], ef[0] + qf[0] * ef[1] * det * el[0])

    def up(row):
        return jnp.broadcast_to(row, (S, L))

    def pair_data(c, v):
        f_mine, f_other = fl_send[c, 0, v], fl_recv[c, 0, v]
        l_mine, l_other = fl_send[c, 1, v], fl_recv[c, 1, v]
        f0, f1 = jnp.where(first_core, f_mine, f_other), jnp.where(first_core, f_other, f_mine)
        l0, l1 = jnp.where(first_core, l_mine, l_other), jnp.where(first_core, l_other, l_mine)
        return f0, f1, l0, l1

    def merge(c):
        fl_copy(c).wait_recv()
        for v in range(CV):
            ef, el, qf, ql, det = pair_coefs(v % JB)
            f0, f1, l0, l1 = pair_data(c, v)
            last0 = up(det) * (l0 + up(ql[0]) * f1)
            first1 = f1 + up(ef[1]) * last0
            lam_send[c, v] = jnp.where(first_chip, l1 + up(el[1]) * last0, f0 + up(qf[0]) * first1)
        lam_copy(c).start()

    def settle(c):
        lam_copy(c).wait_recv()
        for v in range(CV):
            jb = v % JB
            ef, el, qf, ql, det = pair_coefs(jb)
            f0, f1, l0, l1 = pair_data(c, v)
            mu_mine, mu_other = mu_send[jb], mu_recv[jb]
            mid = (lam_recv[c, v] + mu_other * lam_send[c, v]) / (1.0 - mu_mine * mu_other)
            zero = jnp.zeros_like(mid)
            prev, nxt = jnp.where(first_chip, zero, mid), jnp.where(first_chip, mid, zero)
            rest = f1 + up(qf[1]) * nxt
            last0 = up(det) * (l0 + up(el[0]) * prev + up(ql[0]) * rest)
            first1 = rest + up(ef[1]) * last0
            wprev[c, v] = jnp.where(first_core, prev, last0)
            wnext[c, v] = jnp.where(first_core, first1, nxt)

    def x_backward(c):
        prevs = [wprev[c, v] for v in range(CV)]

        def step(t, ws):
            i = NI - 1 - t
            fill = [bcast_x(f_x, i, jb) for jb in range(JB)]
            p = [bcast_x(p_x, i, jb) for jb in range(JB)]
            out = []
            for v in range(CV):
                jb = v % JB
                w = b3[c * CV + v, i] + fill[jb] * prevs[v] - p[jb] * ws[v]
                b1[c * CV + v, i] = w + (w - b1[c * CV + v, i])
                out.append(w)
            return tuple(out)

        lax.fori_loop(0, NI, step, tuple(wnext[c, v] for v in range(CV)), unroll=4)

    def turn(fb):
        for jb in range(JB):
            view = b1.at[fb * JB + jb].reshape(NI * S, L)
            for f in range(S):
                g_out[fb, pl.ds(jb * L * S + f, L, stride=S), :] = view[pl.ds(f, NI, stride=S), :].T

    for c in range(CH):
        for fb in range(c * CB, (c + 1) * CB):
            halo_copy(fb).wait_recv()
            lax.fori_loop(0, S, stencil, fb, unroll=4)
        x_forward(c)
        if c == 0:
            coef_copy.wait_recv()
            for jb in range(JB):
                mu_send[jb] = up(own_mu(jb))
            mu_copy.start()
        else:
            merge(c - 1)
    merge(CH - 1)
    mu_copy.wait_recv()
    for c in range(CH):
        settle(c)
        x_backward(c)
        for fb in range(c * CB, (c + 1) * CB):
            turn(fb)

    def y_forward(t, gs):
        j = jnp.where(first_y, t, NJ - 1 - t)
        inv, s = bcast(inv_t, j), bcast(s_t, j)
        rows = pl.ds(pl.multiple_of(j * S, S), S)
        out = []
        for fb in range(FB):
            g = g_out[fb, rows, :] * inv - s * gs[fb]
            g_out[fb, rows, :] = g
            out.append(g)
        return tuple(out)

    gs = lax.fori_loop(0, NJ, y_forward, tuple(jnp.zeros((S, L), f32) for _ in range(FB)), unroll=4)
    for fb in range(FB):
        yl_send[fb] = gs[fb]
    yl_send[FB] = up(-p_end)
    y_copy = pltpu.make_async_remote_copy(
        yl_send, yl_recv, y_ss, y_rs, device_id=beside, device_id_type=MESH)
    y_copy.start()
    y_copy.wait_recv()
    mu_mine, mu_other = yl_send[FB], yl_recv[FB]
    scale = 1.0 / (1.0 - mu_mine * mu_other)
    for fb in range(FB):
        edge_out[fb] = (yl_recv[fb] + mu_other * yl_send[fb]) * scale

    y_copy.wait_send()
    coef_copy.wait_send()
    mu_copy.wait_send()
    for fb in range(FB):
        halo_copy(fb).wait_send()
    for c in range(CH):
        fl_copy(c).wait_send()
        lam_copy(c).wait_send()


OB = 4


def finish_kernel(g_ref, edge_ref, ratio_ref, out_hbm, buf, out_sem):
    first_y = lax.axis_index("y") == 0

    def out_copy(fb, jb):
        k = fb * JB + jb
        return pltpu.make_async_copy(
            buf.at[k], out_hbm.at[:, pl.ds(fb * S, S), pl.ds(jb * L, L)], out_sem.at[k])

    for start in range(0, FB, OB):
        fbs = range(start, start + OB)

        def y_backward(t, ws):
            j = jnp.where(first_y, NJ - 1 - t, t)
            p = bcast(ratio_ref, j)
            rows = pl.ds(pl.multiple_of(j * S, S), S)
            out = []
            for fb, w in zip(fbs, ws):
                w = g_ref[fb, rows, :] - p * w
                g_ref[fb, rows, :] = w
                out.append(w)
            return tuple(out)

        lax.fori_loop(0, NJ, y_backward, tuple(edge_ref[fb] for fb in fbs), unroll=4)
        for fb in fbs:
            for jb in range(JB):
                view = buf.at[fb * JB + jb].reshape(NI * S, L)
                for f in range(S):
                    view[pl.ds(f, NI, stride=S), :] = g_ref[fb, pl.ds(jb * L * S + f, L, stride=S), :].T
                out_copy(fb, jb).start()
    for fb in range(FB):
        for jb in range(JB):
            out_copy(fb, jb).wait()


def solution(mesh):
    tile_spec = P(("batch", "x"), "y", None)
    coef_spec = P(("batch", "x"), "y")
    vmem = pl.BlockSpec(memory_space=pltpu.VMEM)
    hbm = pl.BlockSpec(memory_space=pl.ANY)
    V, DMA = pltpu.VMEM, pltpu.SemaphoreType.DMA
    row_x, col_t = V((JB, NI, L), f32), V((NJ, NI), f32)

    def local_step(field, *coefs):
        g, edge, ratio = pl.pallas_call(
            reduce_kernel,
            out_shape=(jax.ShapeDtypeStruct((FB, NJ * S, L), f32),
                       jax.ShapeDtypeStruct((FB, S, L), f32),
                       jax.ShapeDtypeStruct((NJ, L), f32)),
            in_specs=[hbm] + [vmem] * 6,
            out_specs=(vmem, vmem, vmem),
            scratch_shapes=[
                V((FB * JB, NI, S, L), f32), V((NF, NJ + 2 * HR, L), f32), V((FB * JB, NI, S, L), f32),
                V((NF, L), f32), V((NF, L), f32),
                row_x, row_x, row_x, row_x, row_x, row_x, row_x, row_x,
                col_t, col_t, col_t, col_t, col_t, col_t, col_t, col_t,
                V((JB, S, L), f32), V((JB, S, L), f32), V((JB, S, L), f32), V((JB, S, L), f32),
                V((CH, 2, CV, S, L), f32), V((CH, 2, CV, S, L), f32),
                V((CH, CV, S, L), f32), V((CH, CV, S, L), f32),
                V((CH, CV, S, L), f32), V((CH, CV, S, L), f32),
                V((FB + 1, S, L), f32), V((FB + 1, S, L), f32),
                DMA((FB * JB,)), DMA((FB,)), DMA((FB,)), DMA, DMA, DMA, DMA,
                DMA((CH,)), DMA((CH,)), DMA((CH,)), DMA((CH,)), DMA, DMA,
            ],
            compiler_params=pltpu.CompilerParams(
                collective_id=0, has_side_effects=True, vmem_limit_bytes=50 << 20),
            name="reduce",
        )(jnp.swapaxes(field, 1, 2), *coefs)
        out = pl.pallas_call(
            finish_kernel,
            out_shape=jax.ShapeDtypeStruct((NI, NF, NJ), f32),
            in_specs=[vmem, vmem, vmem],
            out_specs=hbm,
            scratch_shapes=[V((FB * JB, NI, S, L), f32), DMA((FB * JB,))],
            compiler_params=pltpu.CompilerParams(vmem_limit_bytes=30 << 20),
            name="finish",
        )(g, edge, ratio)
        return jnp.swapaxes(out, 1, 2)

    return jax.shard_map(local_step, mesh=mesh, in_specs=(tile_spec,) + (coef_spec,) * 6,
                         out_specs=tile_spec, check_vma=False)
```

```python
import functools

import jax
import jax.numpy as jnp
from jax import lax
from jax.experimental import pallas as pl
from jax.experimental.pallas import tpu as pltpu
from jax.sharding import PartitionSpec as P

MESH = pl.DeviceIdType.MESH
NI, NF, NJ = 128, 64, 256
L, S = 128, 8
FB = NF // S
JB = NJ // L
CH = 4
CB = FB // CH
CV = CB * JB
HR = 8
f32 = jnp.float32
RL, FL = 38_000_000, 6


def bcast(ref, row):
    return jnp.broadcast_to(ref[pl.ds(row, 1), :], (S, L))


def bcast_x(ref, row, jb):
    return jnp.broadcast_to(ref[jb, pl.ds(row, 1), :], (S, L))


HB = FB // 2
HC = CH // 2


def y_eliminate(first_y, g_ref, inv_t, s_t, last_ref, slots):
    U = 8

    def run(ascending):
        def group(t, gs):
            base = pl.multiple_of(t * U if ascending else NJ - U - t * U, U)
            for r in range(U) if ascending else range(U - 1, -1, -1):
                inv, s = bcast(inv_t, base + r), bcast(s_t, base + r)
                rows = pl.ds(base * S + r * S, S)
                new = []
                for fb in range(HB):
                    g = g_ref[fb, rows, :] * inv - s * gs[fb]
                    g_ref[fb, rows, :] = g
                    new.append(g)
                gs = tuple(new)
            return gs

        gs = lax.fori_loop(0, NJ // U, group, tuple(jnp.zeros((S, L), f32) for _ in range(HB)))
        for fb in range(HB):
            last_ref[slots + fb] = gs[fb]

    pl.when(first_y)(lambda: run(True))
    pl.when(jnp.logical_not(first_y))(lambda: run(False))


def y_substitute(first_y, g_ref, ratio_ref, edges):
    U = 8

    def run(ascending):
        def group(t, ws):
            base = pl.multiple_of(t * U if ascending else NJ - U - t * U, U)
            for r in range(U) if ascending else range(U - 1, -1, -1):
                p = bcast(ratio_ref, base + r)
                rows = pl.ds(base * S + r * S, S)
                new = []
                for fb in range(HB):
                    w = g_ref[fb, rows, :] - p * ws[fb]
                    g_ref[fb, rows, :] = w
                    new.append(w)
                ws = tuple(new)
            return ws

        lax.fori_loop(0, NJ // U, group, tuple(edges))

    pl.when(jnp.logical_not(first_y))(lambda: run(True))
    pl.when(first_y)(lambda: run(False))


def to_rows(g_ref, fb, out_ref):
    for jb in range(JB):
        view = out_ref.at[fb * JB + jb].reshape(NI * S, L)
        for f in range(S):
            view[pl.ds(f, NI, stride=S), :] = g_ref[fb, pl.ds(jb * L * S + f, L, stride=S), :].T


def reduce_kernel(u_hbm, sub_x, diag_x, sup_x, sub_y, diag_y, sup_y,
                  done_a, g_b, edge_out, ratio_out,
                  b1, b2, b3, g_a, halo_send, halo_recv,
                  low_x, cen_x, high_x, inv_x, s_x, p_x, f_x, q_x,
                  sy, dy, uy, cen_t, lo_t, hi_t, b_t, a_t, c_t, inv_t, s_t,
                  coef_send, coef_recv, mu_send, mu_recv,
                  fl_send, fl_recv, lam_send, lam_recv, wprev, wnext,
                  yl_send, yl_recv, ymu_send, ymu_recv,
                  cf_sem, in_sem, halo_ss, halo_rs, coef_ss, coef_rs, mu_ss, mu_rs,
                  fl_ss, fl_rs, lam_ss, lam_rs, y_ss, y_rs):
    my_x = lax.axis_index("x")
    my_y = lax.axis_index("y")
    core = lax.rem(my_x, 2)
    chip = my_x // 2
    mate = {"x": my_x + 1 - 2 * core}
    across = {"x": lax.rem(my_x + 2, 4)}
    beside = {"y": 1 - my_y}
    first_core = core == 0
    first_chip = chip == 0
    first_y = my_y == 0

    cf_copies = []
    for src, dst in ((sub_y, sy), (diag_y, dy), (sup_y, uy)):
        cf_copies.append(pltpu.make_async_copy(src, dst, cf_sem.at[len(cf_copies)]))
    for src, dst in ((sub_x, low_x), (diag_x, cen_x), (sup_x, high_x)):
        for jb in range(JB):
            cf_copies.append(pltpu.make_async_copy(
                src.at[:, pl.ds(jb * L, L)], dst.at[jb], cf_sem.at[len(cf_copies)]))
    for copy in cf_copies:
        copy.start()

    def in_copy(fb, jb):
        k = fb * JB + jb
        return pltpu.make_async_copy(
            u_hbm.at[:, pl.ds(fb * S, S), pl.ds(jb * L, L)], b1.at[k], in_sem.at[k])

    for fb in range(FB):
        for jb in range(JB):
            in_copy(fb, jb).start()

    barrier = pltpu.get_barrier_semaphore()
    for peer in (mate, across, beside):
        pl.semaphore_signal(barrier, inc=1, device_id=peer, device_id_type=MESH)

    for copy in cf_copies:
        copy.wait()
    for jb in range(JB):
        cols = slice(jb * L, (jb + 1) * L)
        d = dy[:, cols].T
        lo = sy[:, cols].T
        hi = uy[:, cols].T
        cen_t[cols, :] = 1.0 - d
        b_t[cols, :] = 1.0 + d
        lo_t[cols, :] = lo
        hi_t[cols, :] = hi
        a_t[cols, :] = jnp.where(first_y, lo, hi)
        c_t[cols, :] = jnp.where(first_y, hi, lo)

    def x_factor(row, state):
        out = []
        for jb in range(JB):
            p_prev, f_prev, q, e_sum = state[jb]
            sub, sup = low_x[jb, row, :], high_x[jb, row, :]
            inv = 1.0 / (1.0 + cen_x[jb, row, :] - sub * p_prev)
            p, s = sup * inv, sub * inv
            fill = -s * f_prev
            inv_x[jb, row, :] = inv
            s_x[jb, row, :] = s
            p_x[jb, row, :] = p
            f_x[jb, row, :] = fill
            q_x[jb, row, :] = q
            out.append((p, fill, -q * p, e_sum + q * fill))
        return tuple(out)

    def y_factor(t, p_prev):
        row = pl.ds(jnp.where(first_y, t, NJ - 1 - t), 1)
        low = a_t[row, :]
        inv = 1.0 / (b_t[row, :] - low * p_prev)
        p = c_t[row, :] * inv
        inv_t[row, :] = inv
        s_t[row, :] = low * inv
        ratio_out[row, :] = p
        return p

    pl.semaphore_wait(barrier, 3)

    def halo_copy(fb):
        rows = pl.ds(pl.multiple_of(fb * S, S), S)
        return pltpu.make_async_remote_copy(
            halo_send.at[rows, :], halo_recv.at[rows, :], halo_ss.at[fb], halo_rs.at[fb],
            device_id=beside, device_id_type=MESH)

    def to_columns(fb, state):
        x_state, p = state
        for jb in range(JB):
            in_copy(fb, jb).wait()
        views = [b1.at[fb * JB + jb].reshape(NI * S, L) for jb in range(JB)]
        for f in range(S):
            parts = [views[jb][pl.ds(f, NI, stride=S), :].T for jb in range(JB)]
            for jb in range(JB):
                b2[fb * S + f, HR + jb * L:HR + (jb + 1) * L, :] = parts[jb]
            halo_send[pl.ds(fb * S + f, 1), :] = jnp.where(
                first_y, parts[JB - 1][L - 1:L, :], parts[0][0:1, :])
        for r in range(NI // FB):
            x_state = x_factor(pl.ds(fb * (NI // FB) + r, 1), x_state)
        for r in range(NJ // FB):
            p = y_factor(fb * (NJ // FB) + r, p)
        halo_copy(fb).start()
        return x_state, p

    none = jnp.zeros((1, L), f32)
    ends, p_end = lax.fori_loop(0, FB, to_columns, (((none, none + 1.0, none + 1.0, none),) * JB, none))
    for jb in range(JB):
        p_last, f_last, q_all, e_sum = ends[jb]
        for r, value in enumerate((e_sum, f_last, q_all, -p_last)):
            coef_send[jb, r:r + 1, :] = value
        coef_send[jb, 4:8, :] = jnp.zeros((4, L), f32)
    ymu_send[...] = jnp.broadcast_to(-p_end, (S, L))
    coef_copy = pltpu.make_async_remote_copy(
        coef_send, coef_recv, coef_ss, coef_rs, device_id=mate, device_id_type=MESH)
    ymu_copy = pltpu.make_async_remote_copy(
        ymu_send, ymu_recv, y_ss.at[2], y_rs.at[2], device_id=beside, device_id_type=MESH)

    def stencil(fi, fb):
        f_all = fb * S + fi
        halo = halo_recv[pl.ds(f_all, 1), :]
        none = jnp.zeros_like(halo)
        b2[f_all, HR - 1:HR, :] = jnp.where(first_y, none, halo)
        b2[f_all, HR + NJ:HR + NJ + 1, :] = jnp.where(first_y, halo, none)
        for jb in range(JB):
            base = HR + jb * L
            cols = slice(jb * L, (jb + 1) * L)
            before = b2[f_all, base - 1:base - 1 + L, :]
            here = b2[f_all, base:base + L, :]
            after = b2[f_all, base + 1:base + 1 + L, :]
            r = cen_t[cols, :] * here - lo_t[cols, :] * before - hi_t[cols, :] * after
            b1.at[fb * JB + jb].reshape(NI * S, L)[pl.ds(fi, NI, stride=S), :] = r.T
        return fb

    def fl_copy(c):
        return pltpu.make_async_remote_copy(
            fl_send.at[c], fl_recv.at[c], fl_ss.at[c], fl_rs.at[c], device_id=mate, device_id_type=MESH)

    def lam_copy(c):
        return pltpu.make_async_remote_copy(
            lam_send.at[c], lam_recv.at[c], lam_ss.at[c], lam_rs.at[c], device_id=across, device_id_type=MESH)

    mu_copy = pltpu.make_async_remote_copy(
        mu_send, mu_recv, mu_ss, mu_rs, device_id=across, device_id_type=MESH)

    def x_forward(c):
        U = 8

        def group(t, state):
            base = pl.multiple_of(t * U, U)
            gs, accs = state
            for r in range(U):
                inv = [bcast_x(inv_x, base + r, jb) for jb in range(JB)]
                s = [bcast_x(s_x, base + r, jb) for jb in range(JB)]
                q = [bcast_x(q_x, base + r, jb) for jb in range(JB)]
                new_g, new_acc = [], []
                for v in range(CV):
                    jb = v % JB
                    g = b1[c * CV + v, base + r] * inv[jb] - s[jb] * gs[v]
                    b3[c * CV + v, base + r] = g
                    new_g.append(g)
                    new_acc.append(accs[v] + q[jb] * g)
                gs, accs = tuple(new_g), tuple(new_acc)
            return gs, accs

        zeros = tuple(jnp.zeros((S, L), f32) for _ in range(CV))
        gs, accs = lax.fori_loop(0, NI // U, group, (zeros, zeros))
        for v in range(CV):
            fl_send[c, 0, v] = accs[v]
            fl_send[c, 1, v] = gs[v]
        fl_copy(c).start()

    def pair_coefs(jb):
        def both(row):
            mine, other = coef_send[jb, row:row + 1, :], coef_recv[jb, row:row + 1, :]
            return jnp.where(first_core, mine, other), jnp.where(first_core, other, mine)

        ef, el, qf, ql = both(0), both(1), both(2), both(3)
        return ef, el, qf, ql, 1.0 / (1.0 - ql[0] * ef[1])

    def own_mu(jb):
        ef, el, qf, ql, det = pair_coefs(jb)
        return jnp.where(first_chip, el[1] * det * ql[0] * qf[1] + ql[1], ef[0] + qf[0] * ef[1] * det * el[0])

    def up(row):
        return jnp.broadcast_to(row, (S, L))

    def pair_data(c, v):
        f_mine, f_other = fl_send[c, 0, v], fl_recv[c, 0, v]
        l_mine, l_other = fl_send[c, 1, v], fl_recv[c, 1, v]
        f0, f1 = jnp.where(first_core, f_mine, f_other), jnp.where(first_core, f_other, f_mine)
        l0, l1 = jnp.where(first_core, l_mine, l_other), jnp.where(first_core, l_other, l_mine)
        return f0, f1, l0, l1

    def merge(c):
        fl_copy(c).wait_recv()
        for v in range(CV):
            ef, el, qf, ql, det = pair_coefs(v % JB)
            f0, f1, l0, l1 = pair_data(c, v)
            last0 = up(det) * (l0 + up(ql[0]) * f1)
            first1 = f1 + up(ef[1]) * last0
            lam_send[c, v] = jnp.where(first_chip, l1 + up(el[1]) * last0, f0 + up(qf[0]) * first1)
        lam_copy(c).start()

    def settle(c):
        lam_copy(c).wait_recv()
        for v in range(CV):
            jb = v % JB
            ef, el, qf, ql, det = pair_coefs(jb)
            f0, f1, l0, l1 = pair_data(c, v)
            mu_mine, mu_other = mu_send[jb], mu_recv[jb]
            mid = (lam_recv[c, v] + mu_other * lam_send[c, v]) / (1.0 - mu_mine * mu_other)
            zero = jnp.zeros_like(mid)
            prev, nxt = jnp.where(first_chip, zero, mid), jnp.where(first_chip, mid, zero)
            rest = f1 + up(qf[1]) * nxt
            last0 = up(det) * (l0 + up(el[0]) * prev + up(ql[0]) * rest)
            first1 = rest + up(ef[1]) * last0
            wprev[c, v] = jnp.where(first_core, prev, last0)
            wnext[c, v] = jnp.where(first_core, first1, nxt)

    def x_backward(c):
        U = 8
        prevs = [wprev[c, v] for v in range(CV)]

        def group(t, ws):
            base = pl.multiple_of(NI - U - t * U, U)
            for r in range(U - 1, -1, -1):
                fill = [bcast_x(f_x, base + r, jb) for jb in range(JB)]
                p = [bcast_x(p_x, base + r, jb) for jb in range(JB)]
                new = []
                for v in range(CV):
                    jb = v % JB
                    w = b3[c * CV + v, base + r] + fill[jb] * prevs[v] - p[jb] * ws[v]
                    b1[c * CV + v, base + r] = w + (w - b1[c * CV + v, base + r])
                    new.append(w)
                ws = tuple(new)
            return ws

        lax.fori_loop(0, NI // U, group, tuple(wnext[c, v] for v in range(CV)))

    def turn(fb, g_ref, slot):
        for jb in range(JB):
            view = b1.at[fb * JB + jb].reshape(NI * S, L)
            for f in range(S):
                g_ref[slot, pl.ds(jb * L * S + f, L, stride=S), :] = view[pl.ds(f, NI, stride=S), :].T

    def y_copy(half):
        rows = pl.ds(half * HB, HB)
        return pltpu.make_async_remote_copy(
            yl_send.at[rows], yl_recv.at[rows], y_ss.at[half], y_rs.at[half],
            device_id=beside, device_id_type=MESH)

    def y_edges(half):
        y_copy(half).wait_recv()
        mu_mine, mu_other = ymu_send[...], ymu_recv[...]
        scale = 1.0 / (1.0 - mu_mine * mu_other)
        return [(yl_recv[half * HB + fb] + mu_other * yl_send[half * HB + fb]) * scale for fb in range(HB)]

    for c in range(CH):
        for fb in range(c * CB, (c + 1) * CB):
            halo_copy(fb).wait_recv()
            lax.fori_loop(0, S, stencil, fb, unroll=4)
        if c == 0:
            coef_copy.start()
            ymu_copy.start()
        x_forward(c)
        if c == 0:
            coef_copy.wait_recv()
            for jb in range(JB):
                mu_send[jb] = up(own_mu(jb))
        else:
            if c == 1:
                mu_copy.start()
            merge(c - 1)
    mu_copy.wait_recv()
    for c in range(CH):
        settle(c)
        x_backward(c)
        if c == 0:
            merge(CH - 1)
        for fb in range(c * CB, (c + 1) * CB):
            turn(fb, g_a if c < HC else g_b, fb % HB)
        if c == HC - 1:
            y_eliminate(first_y, g_a, inv_t, s_t, yl_send, 0)
            y_copy(0).start()
    y_eliminate(first_y, g_b, inv_t, s_t, yl_send, HB)
    y_copy(1).start()
    ymu_copy.wait_recv()
    y_substitute(first_y, g_a, ratio_out, y_edges(0))
    for fb in range(HB):
        to_rows(g_a, fb, done_a)
    for fb, value in enumerate(y_edges(1)):
        edge_out[fb] = value

    ymu_copy.wait_send()
    coef_copy.wait_send()
    mu_copy.wait_send()
    for half in range(2):
        y_copy(half).wait_send()
    for fb in range(FB):
        halo_copy(fb).wait_send()
    for c in range(CH):
        fl_copy(c).wait_send()
        lam_copy(c).wait_send()


def finish_kernel(done_a, g_ref, edge_ref, ratio_ref, out_hbm, buf, out_sem):
    first_y = lax.axis_index("y") == 0

    def out_copy(ref, fb, jb, first):
        k = fb * JB + jb
        return pltpu.make_async_copy(
            ref.at[k], out_hbm.at[:, pl.ds((first + fb) * S, S), pl.ds(jb * L, L)],
            out_sem.at[first * JB + k])

    for fb in range(HB):
        for jb in range(JB):
            out_copy(done_a, fb, jb, 0).start()
    y_substitute(first_y, g_ref, ratio_ref, [edge_ref[fb] for fb in range(HB)])
    for fb in range(HB):
        to_rows(g_ref, fb, buf)
        for jb in range(JB):
            out_copy(buf, fb, jb, HB).start()
    for fb in range(HB):
        for jb in range(JB):
            out_copy(done_a, fb, jb, 0).wait()
            out_copy(buf, fb, jb, HB).wait()


def solution(mesh):
    tile_spec = P(("batch", "x"), "y", None)
    coef_spec = P(("batch", "x"), "y")
    vmem = pl.BlockSpec(memory_space=pltpu.VMEM)
    hbm = pl.BlockSpec(memory_space=pltpu.HBM)
    V, DMA = pltpu.VMEM, pltpu.SemaphoreType.DMA
    row_x, col_t = V((JB, NI, L), f32), V((NJ, NI), f32)

    def local_step(field, *coefs):
        done, g, edge, ratio = pl.pallas_call(
            reduce_kernel,
            out_shape=(jax.ShapeDtypeStruct((HB * JB, NI, S, L), f32),
                       jax.ShapeDtypeStruct((HB, NJ * S, L), f32),
                       jax.ShapeDtypeStruct((HB, S, L), f32),
                       jax.ShapeDtypeStruct((NJ, L), f32)),
            in_specs=[hbm] * 7,
            out_specs=(vmem, vmem, vmem, vmem),
            scratch_shapes=[
                V((FB * JB, NI, S, L), f32), V((NF, NJ + 2 * HR, L), f32), V((FB * JB, NI, S, L), f32),
                V((HB, NJ * S, L), f32),
                V((NF, L), f32), V((NF, L), f32),
                row_x, row_x, row_x, row_x, row_x, row_x, row_x, row_x,
                V((NI, NJ), f32), V((NI, NJ), f32), V((NI, NJ), f32),
                col_t, col_t, col_t, col_t, col_t, col_t, col_t, col_t,
                V((JB, S, L), f32), V((JB, S, L), f32), V((JB, S, L), f32), V((JB, S, L), f32),
                V((CH, 2, CV, S, L), f32), V((CH, 2, CV, S, L), f32),
                V((CH, CV, S, L), f32), V((CH, CV, S, L), f32),
                V((CH, CV, S, L), f32), V((CH, CV, S, L), f32),
                V((FB, S, L), f32), V((FB, S, L), f32), V((S, L), f32), V((S, L), f32),
                DMA((9,)), DMA((FB * JB,)), DMA((FB,)), DMA((FB,)), DMA, DMA, DMA, DMA,
                DMA((CH,)), DMA((CH,)), DMA((CH,)), DMA((CH,)), DMA((3,)), DMA((3,)),
            ],
            compiler_params=pltpu.CompilerParams(
                collective_id=0, has_side_effects=True, vmem_limit_bytes=RL),
            name="reduce",
        )(*(pltpu.with_memory_space_constraint(x, pltpu.HBM) for x in (jnp.swapaxes(field, 1, 2), *coefs)))
        out = pl.pallas_call(
            finish_kernel,
            out_shape=jax.ShapeDtypeStruct((NI, NF, NJ), f32),
            in_specs=[vmem] * 4,
            out_specs=hbm,
            scratch_shapes=[V((HB * JB, NI, S, L), f32), DMA((FB * JB,))],
            compiler_params=pltpu.CompilerParams(vmem_limit_bytes=FL << 20),
            name="finish",
        )(done, g, edge, ratio)
        return jnp.swapaxes(out, 1, 2)

    return jax.shard_map(local_step, mesh=mesh, in_specs=(tile_spec,) + (coef_spec,) * 6,
                         out_specs=tile_spec, check_vma=False)
```

```python
import functools

import jax
import jax.numpy as jnp
from jax import lax
from jax.experimental import pallas as pl
from jax.experimental.pallas import tpu as pltpu
from jax.sharding import PartitionSpec as P

MESH = pl.DeviceIdType.MESH
NI, NF, NJ = 128, 64, 256
L, S = 128, 8
FB = NF // S
JB = NJ // L
CH = 4
CB = FB // CH
CV = CB * JB
HR = 8
f32 = jnp.float32
RL, FL = 44_000_000, 6


def spelled(n, body, state):
    return lax.fori_loop(0, n, body, state, unroll=True)


def aligned(i):
    return pl.multiple_of(i, S)


def bcast(ref, row):
    return jnp.broadcast_to(ref[pl.ds(row, 1), :], (HB, S, L))


def bcast_x(ref, row):
    return jnp.broadcast_to(ref[:, pl.ds(row, 1), :], (CB, JB, S, L))


HB = FB // 2
HC = CH // 2


def y_eliminate(first_y, g_ref, inv_t, s_t, last_ref, slots):
    U = 8

    def run(ascending):
        def group(t, gs):
            base = pl.multiple_of(t * U if ascending else NJ - U - t * U, U)

            def row(r, gs):
                j = base + (r if ascending else U - 1 - r)
                rows = pl.ds(aligned(j * S), S)
                gs = g_ref[:, rows, :] * bcast(inv_t, j) - bcast(s_t, j) * gs
                g_ref[:, rows, :] = gs
                return gs

            return spelled(U, row, gs)

        last_ref[slots:slots + HB] = lax.fori_loop(0, NJ // U, group, jnp.zeros((HB, S, L), f32))

    pl.when(first_y)(lambda: run(True))
    pl.when(jnp.logical_not(first_y))(lambda: run(False))


def y_substitute(first_y, g_ref, ratio_ref, edges):
    U = 8

    def run(ascending):
        def group(t, ws):
            base = pl.multiple_of(t * U if ascending else NJ - U - t * U, U)

            def row(r, ws):
                j = base + (r if ascending else U - 1 - r)
                rows = pl.ds(aligned(j * S), S)
                ws = g_ref[:, rows, :] - bcast(ratio_ref, j) * ws
                g_ref[:, rows, :] = ws
                return ws

            return spelled(U, row, ws)

        lax.fori_loop(0, NJ // U, group, edges)

    pl.when(jnp.logical_not(first_y))(lambda: run(True))
    pl.when(first_y)(lambda: run(False))


def to_rows(g_ref, fb, out_ref, after=None):
    for jb in range(JB):
        view = out_ref.at[fb * JB + jb].reshape(NI * S, L)

        def one(f, _):
            view[pl.ds(f, NI, stride=S), :] = g_ref[fb, pl.ds(jb * L * S + f, L, stride=S), :].T
            return 0

        spelled(S, one, 0)
        if after is not None:
            after(jb)


def reduce_kernel(u_hbm, sub_x, diag_x, sup_x, sub_y, diag_y, sup_y,
                  done_a, g_b, edge_out, ratio_out,
                  u_in, b1s, b2, b3s, g_a, halo_send, halo_recv,
                  low_x, cen_x, high_x, inv_x, s_x, p_x, f_x, q_x,
                  sy, dy, uy, cen_t, lo_t, hi_t, b_t, a_t, c_t, inv_t, s_t,
                  coef_send, coef_recv, mu_send, mu_recv,
                  fl_send, fl_recv, lam_send, lam_recv, wprev, wnext,
                  yl_send, yl_recv, ymu_send, ymu_recv,
                  cf_sem, in_sem, halo_ss, halo_rs, coef_ss, coef_rs, mu_ss, mu_rs,
                  fl_ss, fl_rs, lam_ss, lam_rs, y_ss, y_rs):
    my_x = lax.axis_index("x")
    my_y = lax.axis_index("y")
    core = lax.rem(my_x, 2)
    chip = my_x // 2
    mate = {"x": my_x + 1 - 2 * core}
    across = {"x": lax.rem(my_x + 2, 4)}
    beside = {"y": 1 - my_y}
    first_core = core == 0
    first_chip = chip == 0
    first_y = my_y == 0

    cf_copies = []
    for src, dst in ((sub_y, sy), (diag_y, dy), (sup_y, uy)):
        cf_copies.append(pltpu.make_async_copy(src, dst, cf_sem.at[len(cf_copies)]))
    for src, dst in ((sub_x, low_x), (diag_x, cen_x), (sup_x, high_x)):
        for jb in range(JB):
            cf_copies.append(pltpu.make_async_copy(
                src.at[:, pl.ds(jb * L, L)], dst.at[jb], cf_sem.at[len(cf_copies)]))
    for copy in cf_copies:
        copy.start()

    def in_copy(fb, jb):
        return pltpu.make_async_copy(
            u_hbm.at[:, pl.ds(aligned(fb * S), S), pl.ds(jb * L, L)],
            u_in.at[fb, jb], in_sem.at[fb * JB + jb])

    def start_in(fb, _):
        for jb in range(JB):
            in_copy(fb, jb).start()
        return 0

    lax.fori_loop(0, FB, start_in, 0)

    barrier = pltpu.get_barrier_semaphore()
    for peer in (mate, across, beside):
        pl.semaphore_signal(barrier, inc=1, device_id=peer, device_id_type=MESH)

    for copy in cf_copies:
        copy.wait()
    for jb in range(JB):
        cols = slice(jb * L, (jb + 1) * L)
        d = dy[:, cols].T
        lo = sy[:, cols].T
        hi = uy[:, cols].T
        cen_t[cols, :] = 1.0 - d
        b_t[cols, :] = 1.0 + d
        lo_t[cols, :] = lo
        hi_t[cols, :] = hi
        a_t[cols, :] = jnp.where(first_y, lo, hi)
        c_t[cols, :] = jnp.where(first_y, hi, lo)

    def x_factor(i, state):
        row = pl.ds(i, 1)
        p_prev, f_prev, q, e_sum = state
        sub, sup = low_x[:, row, :], high_x[:, row, :]
        inv = 1.0 / (1.0 + cen_x[:, row, :] - sub * p_prev)
        p, s = sup * inv, sub * inv
        fill = -s * f_prev
        inv_x[:, row, :] = inv
        s_x[:, row, :] = s
        p_x[:, row, :] = p
        f_x[:, row, :] = fill
        q_x[:, row, :] = q
        return p, fill, -q * p, e_sum + q * fill

    def y_factor(t, p_prev):
        row = pl.ds(jnp.where(first_y, t, NJ - 1 - t), 1)
        low = a_t[row, :]
        inv = 1.0 / (b_t[row, :] - low * p_prev)
        p = c_t[row, :] * inv
        inv_t[row, :] = inv
        s_t[row, :] = low * inv
        ratio_out[row, :] = p
        return p

    pl.semaphore_wait(barrier, 3)

    def halo_copy(fb):
        rows = pl.ds(pl.multiple_of(fb * S, S), S)
        return pltpu.make_async_remote_copy(
            halo_send.at[rows, :], halo_recv.at[rows, :], halo_ss.at[fb], halo_rs.at[fb],
            device_id=beside, device_id_type=MESH)

    def to_columns(fb, state):
        x_state, p = state
        for jb in range(JB):
            in_copy(fb, jb).wait()
        views = [u_in.at[fb, jb].reshape(NI * S, L) for jb in range(JB)]

        def one(f, _):
            parts = [views[jb][pl.ds(f, NI, stride=S), :].T for jb in range(JB)]
            for jb in range(JB):
                b2[fb * S + f, HR + jb * L:HR + (jb + 1) * L, :] = parts[jb]
            halo_send[pl.ds(fb * S + f, 1), :] = jnp.where(
                first_y, parts[JB - 1][L - 1:L, :], parts[0][0:1, :])
            return 0

        spelled(S, one, 0)
        x_state = spelled(NI // FB, lambda r, st: x_factor(fb * (NI // FB) + r, st), x_state)
        p = spelled(NJ // FB, lambda r, q: y_factor(fb * (NJ // FB) + r, q), p)
        halo_copy(fb).start()
        return x_state, p

    none = jnp.zeros((JB, 1, L), f32)
    (p_last, f_last, q_all, e_sum), p_end = lax.fori_loop(
        0, FB, to_columns, ((none, none + 1.0, none + 1.0, none), none[0]))
    for r, value in enumerate((e_sum, f_last, q_all, -p_last)):
        coef_send[:, r:r + 1, :] = value
    coef_send[:, 4:8, :] = jnp.zeros((JB, 4, L), f32)
    ymu_send[...] = jnp.broadcast_to(-p_end, (S, L))
    coef_copy = pltpu.make_async_remote_copy(
        coef_send, coef_recv, coef_ss, coef_rs, device_id=mate, device_id_type=MESH)
    ymu_copy = pltpu.make_async_remote_copy(
        ymu_send, ymu_recv, y_ss.at[2], y_rs.at[2], device_id=beside, device_id_type=MESH)

    def set_halo(fb):
        def one(f, _):
            halo = halo_recv[pl.ds(fb * S + f, 1), :]
            none = jnp.zeros_like(halo)
            b2[fb * S + f, HR - 1:HR, :] = jnp.where(first_y, none, halo)
            b2[fb * S + f, HR + NJ:HR + NJ + 1, :] = jnp.where(first_y, halo, none)
            return 0

        spelled(S, one, 0)

    def stencil(c, h, fs, jb):
        cols = slice(jb * L, (jb + 1) * L)
        at = HR + jb * L
        cen, lo, hi = cen_t[cols, :], lo_t[cols, :], hi_t[cols, :]
        for f in fs:
            f_all = (c * CB + h) * S + f
            r = (cen * b2[f_all, at:at + L, :] - lo * b2[f_all, at - 1:at - 1 + L, :]
                 - hi * b2[f_all, at + 1:at + 1 + L, :])
            b1s[c].at[h, jb].reshape(NI * S, L)[pl.ds(f, NI, stride=S), :] = r.T

    def fl_copy(c):
        return pltpu.make_async_remote_copy(
            fl_send.at[c], fl_recv.at[c], fl_ss.at[c], fl_rs.at[c], device_id=mate, device_id_type=MESH)

    def lam_copy(c):
        return pltpu.make_async_remote_copy(
            lam_send.at[c], lam_recv.at[c], lam_ss.at[c], lam_rs.at[c], device_id=across, device_id_type=MESH)

    mu_copy = pltpu.make_async_remote_copy(
        mu_send, mu_recv, mu_ss, mu_rs, device_id=across, device_id_type=MESH)

    def x_forward_rows(c, base, n, state):
        def row(r, state):
            i = base + r
            g, acc = state
            g = b1s[c][:, :, i] * bcast_x(inv_x, i) - bcast_x(s_x, i) * g
            b3s[c][:, :, i] = g
            return g, acc + bcast_x(q_x, i) * g

        return spelled(n, row, state)

    def forward_stage(c, nxt):
        if nxt is not None:
            for h in range(CB):
                halo_copy(nxt * CB + h).wait_recv()

        def half(h, state):
            if nxt is not None:
                set_halo(nxt * CB + h)
            span = NI // CB
            parts = S // 2 * JB
            n = span // parts

            def part(k, state):
                for jb in range(JB):
                    if nxt is not None:
                        stencil(nxt, h, (2 * k, 2 * k + 1), jb)
                    if c is not None:
                        state = x_forward_rows(c, h * span + (k * JB + jb) * n, n, state)
                return state

            return spelled(S // 2, part, state)

        zeros = jnp.zeros((CB, JB, S, L), f32)
        g, acc = lax.fori_loop(0, CB, half, (zeros, zeros))
        if c is not None:
            fl_send[c, 0] = acc
            fl_send[c, 1] = g
            fl_copy(c).start()

    def pair_coefs():
        def both(row):
            mine, other = coef_send[:, row:row + 1, :], coef_recv[:, row:row + 1, :]
            return jnp.where(first_core, mine, other), jnp.where(first_core, other, mine)

        ef, el, qf, ql = both(0), both(1), both(2), both(3)
        return ef, el, qf, ql, 1.0 / (1.0 - ql[0] * ef[1])

    def own_mu():
        ef, el, qf, ql, det = pair_coefs()
        return jnp.where(first_chip, el[1] * det * ql[0] * qf[1] + ql[1], ef[0] + qf[0] * ef[1] * det * el[0])

    def up(rows):
        return jnp.broadcast_to(rows, (CB, JB, S, L))

    def pair_data(c):
        f_mine, f_other = fl_send[c, 0], fl_recv[c, 0]
        l_mine, l_other = fl_send[c, 1], fl_recv[c, 1]
        f0, f1 = jnp.where(first_core, f_mine, f_other), jnp.where(first_core, f_other, f_mine)
        l0, l1 = jnp.where(first_core, l_mine, l_other), jnp.where(first_core, l_other, l_mine)
        return f0, f1, l0, l1

    def merge(c):
        fl_copy(c).wait_recv()
        ef, el, qf, ql, det = pair_coefs()
        f0, f1, l0, l1 = pair_data(c)
        last0 = up(det) * (l0 + up(ql[0]) * f1)
        first1 = f1 + up(ef[1]) * last0
        lam_send[c] = jnp.where(first_chip, l1 + up(el[1]) * last0, f0 + up(qf[0]) * first1)
        lam_copy(c).start()

    def settle(c):
        lam_copy(c).wait_recv()
        ef, el, qf, ql, det = pair_coefs()
        f0, f1, l0, l1 = pair_data(c)
        mu_mine, mu_other = mu_send[...], mu_recv[...]
        scale = 1.0 / (1.0 - mu_mine * mu_other)
        mid = (lam_recv[c] + mu_other[None] * lam_send[c]) * scale[None]
        zero = jnp.zeros_like(mid)
        prev, nxt = jnp.where(first_chip, zero, mid), jnp.where(first_chip, mid, zero)
        rest = f1 + up(qf[1]) * nxt
        last0 = up(det) * (l0 + up(el[0]) * prev + up(ql[0]) * rest)
        first1 = rest + up(ef[1]) * last0
        wprev[c] = jnp.where(first_core, prev, last0)
        wnext[c] = jnp.where(first_core, first1, nxt)

    def x_backward_rows(c, base, n, prev, w):
        def row(r, w):
            i = base + (n - 1 - r)
            w = b3s[c][:, :, i] + bcast_x(f_x, i) * prev - bcast_x(p_x, i) * w
            b1s[c][:, :, i] = w + (w - b1s[c][:, :, i])
            return w

        return spelled(n, row, w)

    def backward_stage(c, prior):
        prevs = wprev[c] if c is not None else None

        def half(h, ws):
            span = NI // CB

            def part(f, ws):
                if c is not None:
                    ws = x_backward_rows(c, (CB - 1 - h) * span + (S - 1 - f) * (span // S), span // S, prevs, ws)
                if prior is not None:
                    g_ref = g_a if prior < HC else g_b
                    for jb in range(JB):
                        view = b1s[prior].at[h, jb].reshape(NI * S, L)
                        g_ref[(prior % HC) * CB + h, pl.ds(jb * L * S + f, L, stride=S), :] = (
                            view[pl.ds(f, NI, stride=S), :].T)
                return ws

            return spelled(S, part, ws)

        start = wnext[c] if c is not None else 0
        lax.fori_loop(0, CB, half, start)

    def y_copy(half):
        rows = pl.ds(half * HB, HB)
        return pltpu.make_async_remote_copy(
            yl_send.at[rows], yl_recv.at[rows], y_ss.at[half], y_rs.at[half],
            device_id=beside, device_id_type=MESH)

    def y_edges(half):
        y_copy(half).wait_recv()
        mu_mine, mu_other = ymu_send[...], ymu_recv[...]
        scale = 1.0 / (1.0 - mu_mine * mu_other)
        rows = slice(half * HB, (half + 1) * HB)
        return (yl_recv[rows] + mu_other * yl_send[rows]) * scale

    coef_copy.start()
    ymu_copy.start()
    forward_stage(None, 0)
    forward_stage(0, 1)
    coef_copy.wait_recv()
    mu_send[...] = jnp.broadcast_to(own_mu(), (JB, S, L))
    for c in range(1, CH):
        forward_stage(c, c + 1 if c + 1 < CH else None)
        if c == 1:
            mu_copy.start()
        merge(c - 1)
    mu_copy.wait_recv()
    settle(0)
    backward_stage(0, None)
    merge(CH - 1)
    for c in range(1, CH):
        if c == HC + 1:
            y_eliminate(first_y, g_a, inv_t, s_t, yl_send, 0)
            y_copy(0).start()
        settle(c)
        backward_stage(c, c - 1)
    backward_stage(None, CH - 1)
    y_eliminate(first_y, g_b, inv_t, s_t, yl_send, HB)
    y_copy(1).start()
    ymu_copy.wait_recv()
    y_substitute(first_y, g_a, ratio_out, y_edges(0))
    for fb in range(HB):
        to_rows(g_a, fb, done_a)
    edge_out[...] = y_edges(1)

    ymu_copy.wait_send()
    coef_copy.wait_send()
    mu_copy.wait_send()
    for half in range(2):
        y_copy(half).wait_send()
    for fb in range(FB):
        halo_copy(fb).wait_send()
    for c in range(CH):
        fl_copy(c).wait_send()
        lam_copy(c).wait_send()


def finish_kernel(done_a, g_ref, edge_ref, ratio_ref, out_hbm, buf, out_sem):
    first_y = lax.axis_index("y") == 0

    def out_copy(ref, fb, jb, first):
        k = fb * JB + jb
        return pltpu.make_async_copy(
            ref.at[k], out_hbm.at[:, pl.ds((first + fb) * S, S), pl.ds(jb * L, L)],
            out_sem.at[first * JB + k])

    for fb in range(HB):
        for jb in range(JB):
            out_copy(done_a, fb, jb, 0).start()
    y_substitute(first_y, g_ref, ratio_ref, edge_ref[...])
    for fb in range(HB):
        to_rows(g_ref, fb, buf, lambda jb, fb=fb: out_copy(buf, fb, jb, HB).start())
    for fb in range(HB):
        for jb in range(JB):
            out_copy(done_a, fb, jb, 0).wait()
            out_copy(buf, fb, jb, HB).wait()


def solution(mesh):
    tile_spec = P(("batch", "x"), "y", None)
    coef_spec = P(("batch", "x"), "y")
    vmem = pl.BlockSpec(memory_space=pltpu.VMEM)
    hbm = pl.BlockSpec(memory_space=pltpu.HBM)
    V, DMA = pltpu.VMEM, pltpu.SemaphoreType.DMA
    row_x, col_t = V((JB, NI, L), f32), V((NJ, NI), f32)

    def local_step(field, *coefs):
        done, g, edge, ratio = pl.pallas_call(
            reduce_kernel,
            out_shape=(jax.ShapeDtypeStruct((HB * JB, NI, S, L), f32),
                       jax.ShapeDtypeStruct((HB, NJ * S, L), f32),
                       jax.ShapeDtypeStruct((HB, S, L), f32),
                       jax.ShapeDtypeStruct((NJ, L), f32)),
            in_specs=[hbm] * 7,
            out_specs=(vmem, vmem, vmem, vmem),
            scratch_shapes=[
                V((FB, JB, NI, S, L), f32), [V((CB, JB, NI, S, L), f32)] * CH, V((NF, NJ + 2 * HR, L), f32), [V((CB, JB, NI, S, L), f32)] * CH,
                V((HB, NJ * S, L), f32),
                V((NF, L), f32), V((NF, L), f32),
                row_x, row_x, row_x, row_x, row_x, row_x, row_x, row_x,
                V((NI, NJ), f32), V((NI, NJ), f32), V((NI, NJ), f32),
                col_t, col_t, col_t, col_t, col_t, col_t, col_t, col_t,
                V((JB, S, L), f32), V((JB, S, L), f32), V((JB, S, L), f32), V((JB, S, L), f32),
                V((CH, 2, CB, JB, S, L), f32), V((CH, 2, CB, JB, S, L), f32),
                V((CH, CB, JB, S, L), f32), V((CH, CB, JB, S, L), f32),
                V((CH, CB, JB, S, L), f32), V((CH, CB, JB, S, L), f32),
                V((FB, S, L), f32), V((FB, S, L), f32), V((S, L), f32), V((S, L), f32),
                DMA((9,)), DMA((FB * JB,)), DMA((FB,)), DMA((FB,)), DMA, DMA, DMA, DMA,
                DMA((CH,)), DMA((CH,)), DMA((CH,)), DMA((CH,)), DMA((3,)), DMA((3,)),
            ],
            compiler_params=pltpu.CompilerParams(
                collective_id=0, has_side_effects=True, vmem_limit_bytes=RL),
            name="reduce",
        )(*(pltpu.with_memory_space_constraint(x, pltpu.HBM) for x in (jnp.swapaxes(field, 1, 2), *coefs)))
        out = pl.pallas_call(
            finish_kernel,
            out_shape=jax.ShapeDtypeStruct((NI, NF, NJ), f32),
            in_specs=[vmem] * 4,
            out_specs=hbm,
            scratch_shapes=[V((HB * JB, NI, S, L), f32), DMA((FB * JB,))],
            compiler_params=pltpu.CompilerParams(vmem_limit_bytes=FL << 20),
            name="finish",
        )(done, g, edge, ratio)
        return jnp.swapaxes(out, 1, 2)

    return jax.shard_map(local_step, mesh=mesh, in_specs=(tile_spec,) + (coef_spec,) * 6,
                         out_specs=tile_spec, check_vma=False)
```

```python
import functools

import jax
import jax.numpy as jnp
from jax import lax
from jax.experimental import pallas as pl
from jax.experimental.pallas import tpu as pltpu
from jax.sharding import PartitionSpec as P

MESH = pl.DeviceIdType.MESH
NI, NF, NJ = 128, 64, 256
L, S = 128, 8
FB = NF // S
JB = NJ // L
CH = 4
CB = FB // CH
CV = CB * JB
HR = 8
HW = NJ + 2 * HR
f32 = jnp.float32
RL, FL = 42_500_000, 6
LAG = 1
PITCH = 12


def spelled(n, body, state):
    return lax.fori_loop(0, n, body, state, unroll=True)


def aligned(i):
    return pl.multiple_of(i, S)


def bcast(ref, row):
    return jnp.broadcast_to(ref[pl.ds(row, 1), :], (HB, S, L))


def bcast_x(ref, row):
    return jnp.broadcast_to(ref[:, pl.ds(row, 1), :], (CB, JB, S, L))


HB = FB // 2
HC = CH // 2


def y_eliminate(first_y, g_ref, inv_t, s_t, last_ref, slots):
    U = 8

    def run(ascending):
        def group(t, gs):
            base = pl.multiple_of(t * U if ascending else NJ - U - t * U, U)

            def row(r, gs):
                j = base + (r if ascending else U - 1 - r)
                rows = pl.ds(j * PITCH, S)
                gs = g_ref[:, rows, :] * bcast(inv_t, j) - bcast(s_t, j) * gs
                g_ref[:, rows, :] = gs
                return gs

            return spelled(U, row, gs)

        last_ref[slots:slots + HB] = lax.fori_loop(0, NJ // U, group, jnp.zeros((HB, S, L), f32))

    pl.when(first_y)(lambda: run(True))
    pl.when(jnp.logical_not(first_y))(lambda: run(False))


def y_substitute(first_y, g_ref, ratio_ref, edges):
    U = 8

    def run(ascending):
        def group(t, ws):
            base = pl.multiple_of(t * U if ascending else NJ - U - t * U, U)

            def row(r, ws):
                j = base + (r if ascending else U - 1 - r)
                rows = pl.ds(j * PITCH, S)
                ws = g_ref[:, rows, :] - bcast(ratio_ref, j) * ws
                g_ref[:, rows, :] = ws
                return ws

            return spelled(U, row, ws)

        lax.fori_loop(0, NJ // U, group, edges)

    pl.when(jnp.logical_not(first_y))(lambda: run(True))
    pl.when(first_y)(lambda: run(False))


def to_rows(g_ref, fb, out_ref, after=None):
    for jb in range(JB):
        view = out_ref.at[fb * JB + jb].reshape(NI * S, L)

        def one(f, _):
            view[pl.ds(f, NI, stride=S), :] = g_ref[fb, pl.ds(jb * L * PITCH + f, L, stride=PITCH), :].T
            return 0

        spelled(S, one, 0)
        if after is not None:
            after(jb)


def reduce_kernel(u_hbm, sub_x, diag_x, sup_x, sub_y, diag_y, sup_y,
                  done_a, g_b, edge_out, ratio_out,
                  u_in, b1s, b2, b3s, halo_send, halo_recv,
                  low_x, cen_x, high_x, inv_x, s_x, p_x, f_x, q_x,
                  sy, dy, uy, cen_t, lo_t, hi_t, b_t, a_t, c_t, inv_t, s_t,
                  coef_send, coef_recv, mu_send, mu_recv,
                  fl_send, fl_recv, lam_send, lam_recv, wprev, wnext,
                  yl_send, yl_recv, ymu_send, ymu_recv,
                  cf_sem, in_sem, halo_ss, halo_rs, coef_ss, coef_rs, mu_ss, mu_rs,
                  fl_ss, fl_rs, lam_ss, lam_rs, y_ss, y_rs):
    my_x = lax.axis_index("x")
    my_y = lax.axis_index("y")
    core = lax.rem(my_x, 2)
    chip = my_x // 2
    mate = {"x": my_x + 1 - 2 * core}
    across = {"x": lax.rem(my_x + 2, 4)}
    beside = {"y": 1 - my_y}
    first_core = core == 0
    first_chip = chip == 0
    first_y = my_y == 0

    cf_copies = []
    for src, dst in ((sub_y, sy), (diag_y, dy), (sup_y, uy)):
        cf_copies.append(pltpu.make_async_copy(src, dst, cf_sem.at[len(cf_copies)]))
    for src, dst in ((sub_x, low_x), (diag_x, cen_x), (sup_x, high_x)):
        for jb in range(JB):
            cf_copies.append(pltpu.make_async_copy(
                src.at[:, pl.ds(jb * L, L)], dst.at[jb], cf_sem.at[len(cf_copies)]))
    for copy in cf_copies:
        copy.start()

    def in_copy(fb, jb):
        return pltpu.make_async_copy(
            u_hbm.at[:, pl.ds(aligned(fb * S), S), pl.ds(jb * L, L)],
            u_in.at[fb, jb], in_sem.at[fb * JB + jb])

    def start_in(fb, _):
        for jb in range(JB):
            in_copy(fb, jb).start()
        return 0

    lax.fori_loop(0, FB, start_in, 0)

    barrier = pltpu.get_barrier_semaphore()
    for peer in (mate, across, beside):
        pl.semaphore_signal(barrier, inc=1, device_id=peer, device_id_type=MESH)

    for copy in cf_copies:
        copy.wait()
    for jb in range(JB):
        cols = slice(jb * L, (jb + 1) * L)
        d = dy[:, cols].T
        lo = sy[:, cols].T
        hi = uy[:, cols].T
        cen_t[cols, :] = 1.0 - d
        b_t[cols, :] = 1.0 + d
        lo_t[cols, :] = lo
        hi_t[cols, :] = hi
        a_t[cols, :] = jnp.where(first_y, lo, hi)
        c_t[cols, :] = jnp.where(first_y, hi, lo)

    def x_factor(i, state):
        row = pl.ds(i, 1)
        p_prev, f_prev, q, e_sum = state
        sub, sup = low_x[:, row, :], high_x[:, row, :]
        inv = 1.0 / (1.0 + cen_x[:, row, :] - sub * p_prev)
        p, s = sup * inv, sub * inv
        fill = -s * f_prev
        inv_x[:, row, :] = inv
        s_x[:, row, :] = s
        p_x[:, row, :] = p
        f_x[:, row, :] = fill
        q_x[:, row, :] = q
        return p, fill, -q * p, e_sum + q * fill

    def y_factor(t, p_prev):
        row = pl.ds(jnp.where(first_y, t, NJ - 1 - t), 1)
        low = a_t[row, :]
        inv = 1.0 / (b_t[row, :] - low * p_prev)
        p = c_t[row, :] * inv
        inv_t[row, :] = inv
        s_t[row, :] = low * inv
        ratio_out[row, :] = p
        return p

    pl.semaphore_wait(barrier, 3)

    def halo_copy(fb):
        rows = pl.ds(pl.multiple_of(fb * S, S), S)
        return pltpu.make_async_remote_copy(
            halo_send.at[rows, :], halo_recv.at[rows, :], halo_ss.at[fb], halo_rs.at[fb],
            device_id=beside, device_id_type=MESH)

    def to_columns(fb, state):
        x_state, p = state
        for jb in range(JB):
            in_copy(fb, jb).wait()
        views = [u_in.at[fb, jb].reshape(NI * S, L) for jb in range(JB)]

        def one(f, _):
            parts = [views[jb][pl.ds(f, NI, stride=S), :].T for jb in range(JB)]
            for jb in range(JB):
                b2[pl.ds((fb * S + f) * HW + HR + jb * L, L), :] = parts[jb]
            halo_send[pl.ds(fb * S + f, 1), :] = jnp.where(
                first_y, parts[JB - 1][L - 1:L, :], parts[0][0:1, :])
            return 0

        spelled(S, one, 0)
        x_state = spelled(NI // FB, lambda r, st: x_factor(fb * (NI // FB) + r, st), x_state)
        p = spelled(NJ // FB, lambda r, q: y_factor(fb * (NJ // FB) + r, q), p)
        halo_copy(fb).start()
        return x_state, p

    none = jnp.zeros((JB, 1, L), f32)
    (p_last, f_last, q_all, e_sum), p_end = lax.fori_loop(
        0, FB, to_columns, ((none, none + 1.0, none + 1.0, none), none[0]))
    for r, value in enumerate((e_sum, f_last, q_all, -p_last)):
        coef_send[:, r:r + 1, :] = value
    coef_send[:, 4:8, :] = jnp.zeros((JB, 4, L), f32)
    ymu_send[...] = jnp.broadcast_to(-p_end, (S, L))
    coef_copy = pltpu.make_async_remote_copy(
        coef_send, coef_recv, coef_ss, coef_rs, device_id=mate, device_id_type=MESH)
    ymu_copy = pltpu.make_async_remote_copy(
        ymu_send, ymu_recv, y_ss.at[2], y_rs.at[2], device_id=beside, device_id_type=MESH)

    here = my_x < 4
    g_a = b2.at[pl.ds(0, HB * NJ * PITCH), :].reshape(HB, NJ * PITCH, L)

    def paced(value, tag):
        return jnp.where(here, value, tag)

    def set_halo(fb):
        def one(f, _):
            halo = halo_recv[pl.ds(fb * S + f, 1), :]
            none = jnp.zeros_like(halo)
            b2[pl.ds((fb * S + f) * HW + HR - 1, 1), :] = jnp.where(first_y, none, halo)
            b2[pl.ds((fb * S + f) * HW + HR + NJ, 1), :] = jnp.where(first_y, halo, none)
            return 0

        spelled(S, one, 0)

    def stencil(c, h, fs, jb):
        cols = slice(jb * L, (jb + 1) * L)
        cen, lo, hi = cen_t[cols, :], lo_t[cols, :], hi_t[cols, :]
        tags = []
        for f in fs:
            at = ((c * CB + h) * S + f) * HW + HR + jb * L
            r = cen * b2[pl.ds(at, L), :] - lo * b2[pl.ds(at - 1, L), :] - hi * b2[pl.ds(at + 1, L), :]
            rt = r.T
            b1s[c][h, jb, pl.ds(f, NI, stride=PITCH), :] = rt
            tags.append(rt[0:S, :])
        return tags[0]

    def fl_copy(c):
        return pltpu.make_async_remote_copy(
            fl_send.at[c], fl_recv.at[c], fl_ss.at[c], fl_rs.at[c], device_id=mate, device_id_type=MESH)

    def lam_copy(c):
        return pltpu.make_async_remote_copy(
            lam_send.at[c], lam_recv.at[c], lam_ss.at[c], lam_rs.at[c], device_id=across, device_id_type=MESH)

    mu_copy = pltpu.make_async_remote_copy(
        mu_send, mu_recv, mu_ss, mu_rs, device_id=across, device_id_type=MESH)

    def x_forward_rows(c, base, n, state):
        def row(r, state):
            i = base + r
            g, acc = state
            g = b1s[c][:, :, pl.ds(i * PITCH, S), :] * bcast_x(inv_x, i) - bcast_x(s_x, i) * g
            b3s[c][:, :, i] = g
            return g, acc + bcast_x(q_x, i) * g

        return spelled(n, row, state)

    def forward_stage(c, nxt):
        if nxt is not None:
            for h in range(CB):
                halo_copy(nxt * CB + h).wait_recv()

        def half(h, state):
            if nxt is not None:
                set_halo(nxt * CB + h)
            span = NI // CB
            n = span // (S // 2)

            def part(k, carry):
                (g, acc), tag = carry
                new_tag = tag
                if c is not None:
                    if nxt is not None:
                        g = paced(g, tag)
                    g, acc = x_forward_rows(c, h * span + k * n, n, (g, acc))
                if nxt is not None:
                    new_tag = stencil(nxt, h, (2 * k, 2 * k + 1), 0)
                    stencil(nxt, h, (2 * k, 2 * k + 1), 1)
                return (g, acc), new_tag

            return spelled(S // 2, part, (state, jnp.zeros((S, L), f32)))[0]

        zeros = jnp.zeros((CB, JB, S, L), f32)
        g, acc = lax.fori_loop(0, CB, half, (zeros, zeros))
        if c is not None:
            fl_send[c, 0] = acc
            fl_send[c, 1] = g
            fl_copy(c).start()

    def pair_coefs():
        def both(row):
            mine, other = coef_send[:, row:row + 1, :], coef_recv[:, row:row + 1, :]
            return jnp.where(first_core, mine, other), jnp.where(first_core, other, mine)

        ef, el, qf, ql = both(0), both(1), both(2), both(3)
        return ef, el, qf, ql, 1.0 / (1.0 - ql[0] * ef[1])

    def own_mu():
        ef, el, qf, ql, det = pair_coefs()
        return jnp.where(first_chip, el[1] * det * ql[0] * qf[1] + ql[1], ef[0] + qf[0] * ef[1] * det * el[0])

    def up(rows):
        return jnp.broadcast_to(rows, (CB, JB, S, L))

    def pair_data(c):
        f_mine, f_other = fl_send[c, 0], fl_recv[c, 0]
        l_mine, l_other = fl_send[c, 1], fl_recv[c, 1]
        f0, f1 = jnp.where(first_core, f_mine, f_other), jnp.where(first_core, f_other, f_mine)
        l0, l1 = jnp.where(first_core, l_mine, l_other), jnp.where(first_core, l_other, l_mine)
        return f0, f1, l0, l1

    def merge(c):
        fl_copy(c).wait_recv()
        ef, el, qf, ql, det = pair_coefs()
        f0, f1, l0, l1 = pair_data(c)
        last0 = up(det) * (l0 + up(ql[0]) * f1)
        first1 = f1 + up(ef[1]) * last0
        lam_send[c] = jnp.where(first_chip, l1 + up(el[1]) * last0, f0 + up(qf[0]) * first1)
        lam_copy(c).start()

    def settle(c):
        lam_copy(c).wait_recv()
        ef, el, qf, ql, det = pair_coefs()
        f0, f1, l0, l1 = pair_data(c)
        mu_mine, mu_other = mu_send[...], mu_recv[...]
        scale = 1.0 / (1.0 - mu_mine * mu_other)
        mid = (lam_recv[c] + mu_other[None] * lam_send[c]) * scale[None]
        zero = jnp.zeros_like(mid)
        prev, nxt = jnp.where(first_chip, zero, mid), jnp.where(first_chip, mid, zero)
        rest = f1 + up(qf[1]) * nxt
        last0 = up(det) * (l0 + up(el[0]) * prev + up(ql[0]) * rest)
        first1 = rest + up(ef[1]) * last0
        wprev[c] = jnp.where(first_core, prev, last0)
        wnext[c] = jnp.where(first_core, first1, nxt)

    def x_backward_rows(c, base, n, prev, w):
        def row(r, w):
            i = base + (n - 1 - r)
            w = b3s[c][:, :, i] + bcast_x(f_x, i) * prev - bcast_x(p_x, i) * w
            at = pl.ds(i * PITCH, S)
            b1s[c][:, :, at, :] = w + (w - b1s[c][:, :, at, :])
            return w

        return spelled(n, row, w)

    def backward_stage(c, prior):
        prevs = wprev[c] if c is not None else None

        def half(h, ws):
            span = NI // CB

            n = span // (S * JB)

            def part(f, carry):
                ws, tags = carry
                for jb in range(JB):
                    if c is not None:
                        if prior is not None:
                            ws = paced(ws, tags[0])
                        base = (CB - 1 - h) * span + (S * JB - 1 - f * JB - jb) * n
                        ws = x_backward_rows(c, base, n, prevs, ws)
                    if prior is not None:
                        g_ref = g_a if prior < HC else g_b
                        cols = b1s[prior][h, jb, pl.ds(f, NI, stride=PITCH), :].T
                        g_ref[(prior % HC) * CB + h, pl.ds(jb * L * PITCH + f, L, stride=PITCH), :] = cols
                        tags = tags[1:] + (cols[0:S, :],)
                return ws, tags

            return spelled(S, part, (ws, (jnp.zeros((S, L), f32),) * LAG))[0]

        start = wnext[c] if c is not None else 0
        lax.fori_loop(0, CB, half, start)

    def y_copy(half):
        rows = pl.ds(half * HB, HB)
        return pltpu.make_async_remote_copy(
            yl_send.at[rows], yl_recv.at[rows], y_ss.at[half], y_rs.at[half],
            device_id=beside, device_id_type=MESH)

    def y_edges(half):
        y_copy(half).wait_recv()
        mu_mine, mu_other = ymu_send[...], ymu_recv[...]
        scale = 1.0 / (1.0 - mu_mine * mu_other)
        rows = slice(half * HB, (half + 1) * HB)
        return (yl_recv[rows] + mu_other * yl_send[rows]) * scale

    coef_copy.start()
    ymu_copy.start()
    forward_stage(None, 0)
    forward_stage(0, 1)
    coef_copy.wait_recv()
    mu_send[...] = jnp.broadcast_to(own_mu(), (JB, S, L))
    for c in range(1, CH):
        forward_stage(c, c + 1 if c + 1 < CH else None)
        if c == 1:
            mu_copy.start()
        merge(c - 1)
    mu_copy.wait_recv()
    settle(0)
    backward_stage(0, None)
    merge(CH - 1)
    for c in range(1, CH):
        if c == HC + 1:
            y_eliminate(first_y, g_a, inv_t, s_t, yl_send, 0)
            y_copy(0).start()
        settle(c)
        backward_stage(c, c - 1)
    backward_stage(None, CH - 1)
    y_eliminate(first_y, g_b, inv_t, s_t, yl_send, HB)
    y_copy(1).start()
    ymu_copy.wait_recv()
    y_substitute(first_y, g_a, ratio_out, y_edges(0))
    for fb in range(HB):
        to_rows(g_a, fb, done_a)
    edge_out[...] = y_edges(1)

    ymu_copy.wait_send()
    coef_copy.wait_send()
    mu_copy.wait_send()
    for half in range(2):
        y_copy(half).wait_send()
    for fb in range(FB):
        halo_copy(fb).wait_send()
    for c in range(CH):
        fl_copy(c).wait_send()
        lam_copy(c).wait_send()


def finish_kernel(done_a, g_ref, edge_ref, ratio_ref, out_hbm, buf, out_sem):
    first_y = lax.axis_index("y") == 0

    def out_copy(ref, fb, jb, first):
        k = fb * JB + jb
        return pltpu.make_async_copy(
            ref.at[k], out_hbm.at[:, pl.ds((first + fb) * S, S), pl.ds(jb * L, L)],
            out_sem.at[first * JB + k])

    for fb in range(HB):
        for jb in range(JB):
            out_copy(done_a, fb, jb, 0).start()
    y_substitute(first_y, g_ref, ratio_ref, edge_ref[...])
    for fb in range(HB):
        to_rows(g_ref, fb, buf, lambda jb, fb=fb: out_copy(buf, fb, jb, HB).start())
    for fb in range(HB):
        for jb in range(JB):
            out_copy(done_a, fb, jb, 0).wait()
            out_copy(buf, fb, jb, HB).wait()


def solution(mesh):
    tile_spec = P(("batch", "x"), "y", None)
    coef_spec = P(("batch", "x"), "y")
    vmem = pl.BlockSpec(memory_space=pltpu.VMEM)
    hbm = pl.BlockSpec(memory_space=pltpu.HBM)
    V, DMA = pltpu.VMEM, pltpu.SemaphoreType.DMA
    row_x, col_t = V((JB, NI, L), f32), V((NJ, NI), f32)

    def local_step(field, *coefs):
        done, g, edge, ratio = pl.pallas_call(
            reduce_kernel,
            out_shape=(jax.ShapeDtypeStruct((HB * JB, NI, S, L), f32),
                       jax.ShapeDtypeStruct((HB, NJ * PITCH, L), f32),
                       jax.ShapeDtypeStruct((HB, S, L), f32),
                       jax.ShapeDtypeStruct((NJ, L), f32)),
            in_specs=[hbm] * 7,
            out_specs=(vmem, vmem, vmem, vmem),
            scratch_shapes=[
                V((FB, JB, NI, S, L), f32), [V((CB, JB, NI * PITCH, L), f32)] * CH, V((NF * HW, L), f32), [V((CB, JB, NI, S, L), f32)] * CH,
                V((NF, L), f32), V((NF, L), f32),
                row_x, row_x, row_x, row_x, row_x, row_x, row_x, row_x,
                V((NI, NJ), f32), V((NI, NJ), f32), V((NI, NJ), f32),
                col_t, col_t, col_t, col_t, col_t, col_t, col_t, col_t,
                V((JB, S, L), f32), V((JB, S, L), f32), V((JB, S, L), f32), V((JB, S, L), f32),
                V((CH, 2, CB, JB, S, L), f32), V((CH, 2, CB, JB, S, L), f32),
                V((CH, CB, JB, S, L), f32), V((CH, CB, JB, S, L), f32),
                V((CH, CB, JB, S, L), f32), V((CH, CB, JB, S, L), f32),
                V((FB, S, L), f32), V((FB, S, L), f32), V((S, L), f32), V((S, L), f32),
                DMA((9,)), DMA((FB * JB,)), DMA((FB,)), DMA((FB,)), DMA, DMA, DMA, DMA,
                DMA((CH,)), DMA((CH,)), DMA((CH,)), DMA((CH,)), DMA((3,)), DMA((3,)),
            ],
            compiler_params=pltpu.CompilerParams(
                collective_id=0, has_side_effects=True, vmem_limit_bytes=RL),
            name="reduce",
        )(*(pltpu.with_memory_space_constraint(x, pltpu.HBM) for x in (jnp.swapaxes(field, 1, 2), *coefs)))
        out = pl.pallas_call(
            finish_kernel,
            out_shape=jax.ShapeDtypeStruct((NI, NF, NJ), f32),
            in_specs=[vmem] * 4,
            out_specs=hbm,
            scratch_shapes=[V((HB * JB, NI, S, L), f32), DMA((FB * JB,))],
            compiler_params=pltpu.CompilerParams(vmem_limit_bytes=FL << 20),
            name="finish",
        )(done, g, edge, ratio)
        return jnp.swapaxes(out, 1, 2)

    return jax.shard_map(local_step, mesh=mesh, in_specs=(tile_spec,) + (coef_spec,) * 6,
                         out_specs=tile_spec, check_vma=False)
```

```python
import functools

import jax
import jax.numpy as jnp
from jax import lax
from jax.experimental import pallas as pl
from jax.experimental.pallas import tpu as pltpu
from jax.sharding import PartitionSpec as P

MESH = pl.DeviceIdType.MESH
NI, NF, NJ = 128, 64, 256
L, S = 128, 8
FB = NF // S
JB = NJ // L
CH = 4
CB = FB // CH
CV = CB * JB
HR = 8
HW = NJ + 2 * HR
f32 = jnp.float32
RL, FL = 42_500_000, 6
LAG = 1
FP, FLAG = 2, 1
YT = 16
PITCH = 12


def spelled(n, body, state):
    return lax.fori_loop(0, n, body, state, unroll=True)


def aligned(i):
    return pl.multiple_of(i, S)


def bcast(ref, row):
    return jnp.broadcast_to(ref[pl.ds(row, 1), :], (HB, S, L))


def bcast_x(ref, row):
    return jnp.broadcast_to(ref[:, pl.ds(row, 1), :], (CB, JB, S, L))


HB = FB // 2
HC = CH // 2


def y_eliminate(first_y, g_ref, inv_t, s_t, last_ref, slots):
    U = 8

    def run(ascending):
        def group(t, gs):
            base = pl.multiple_of(t * U if ascending else NJ - U - t * U, U)

            def row(r, gs):
                j = base + (r if ascending else U - 1 - r)
                rows = pl.ds(j * PITCH, S)
                gs = g_ref[:, rows, :] * bcast(inv_t, j) - bcast(s_t, j) * gs
                g_ref[:, rows, :] = gs
                return gs

            return spelled(U, row, gs)

        last_ref[slots:slots + HB] = lax.fori_loop(0, NJ // U, group, jnp.zeros((HB, S, L), f32))

    pl.when(first_y)(lambda: run(True))
    pl.when(jnp.logical_not(first_y))(lambda: run(False))


def y_substitute(first_y, g_ref, ratio_ref, edges):
    U = 8

    def run(ascending):
        def group(t, ws):
            base = pl.multiple_of(t * U if ascending else NJ - U - t * U, U)

            def row(r, ws):
                j = base + (r if ascending else U - 1 - r)
                rows = pl.ds(j * PITCH, S)
                ws = g_ref[:, rows, :] - bcast(ratio_ref, j) * ws
                g_ref[:, rows, :] = ws
                return ws

            return spelled(U, row, ws)

        lax.fori_loop(0, NJ // U, group, edges)

    pl.when(jnp.logical_not(first_y))(lambda: run(True))
    pl.when(first_y)(lambda: run(False))


def to_rows(g_ref, fb, out_ref, after=None):
    for jb in range(JB):
        view = out_ref.at[fb * JB + jb].reshape(NI * S, L)

        def one(f, _):
            view[pl.ds(f, NI, stride=S), :] = g_ref[fb, pl.ds(jb * L * PITCH + f, L, stride=PITCH), :].T
            return 0

        spelled(S, one, 0)
        if after is not None:
            after(jb)


def reduce_kernel(u_hbm, sub_x, diag_x, sup_x, sub_y, diag_y, sup_y,
                  done_a, g_b, edge_out, ratio_out,
                  u_in, b1s, b2, b3s, halo_send, halo_recv,
                  low_x, cen_x, high_x, inv_x, s_x, p_x, f_x, q_x,
                  sy, dy, uy, cen_t, lo_t, hi_t, b_t, a_t, c_t, inv_t, s_t,
                  coef_send, coef_recv, mu_send, mu_recv,
                  fl_send, fl_recv, part_send, part_recv, wprev, wnext,
                  yl_send, yl_recv, ymu_send, ymu_recv,
                  cf_sem, in_sem, halo_ss, halo_rs, coef_ss, coef_rs, mu_ss, mu_rs,
                  fl_ss, fl_rs, part_ss, part_rs, y_ss, y_rs):
    my_x = lax.axis_index("x")
    my_y = lax.axis_index("y")
    core = lax.rem(my_x, 2)
    chip = my_x // 2
    mate = {"x": my_x + 1 - 2 * core}
    across = {"x": lax.rem(my_x + 2, 4)}
    beside = {"y": 1 - my_y}
    first_core = core == 0
    first_chip = chip == 0
    first_y = my_y == 0

    def in_copy(fb, jb):
        return pltpu.make_async_copy(
            u_hbm.at[:, pl.ds(aligned(fb * S), S), pl.ds(jb * L, L)],
            u_in.at[fb, jb], in_sem.at[fb * JB + jb])

    def start_in(fb, _):
        for jb in range(JB):
            in_copy(fb, jb).start()
        return 0

    start_in(0, 0)
    cf_copies = []
    for src, dst in ((sub_y, sy), (diag_y, dy), (sup_y, uy)):
        cf_copies.append(pltpu.make_async_copy(src, dst, cf_sem.at[len(cf_copies)]))
    for src, dst in ((sub_x, low_x), (diag_x, cen_x), (sup_x, high_x)):
        for jb in range(JB):
            cf_copies.append(pltpu.make_async_copy(
                src.at[:, pl.ds(jb * L, L)], dst.at[jb], cf_sem.at[len(cf_copies)]))
    for copy in cf_copies:
        copy.start()
    lax.fori_loop(1, FB, start_in, 0)

    barrier = pltpu.get_barrier_semaphore()
    for peer in (mate, across, {"x": lax.rem(my_x + 2, 4) + 1 - 2 * core}, beside):
        pl.semaphore_signal(barrier, inc=1, device_id=peer, device_id_type=MESH)

    def x_factor(i, state):
        row = pl.ds(i, 1)
        p_prev, f_prev, q, e_sum = state
        sub, sup = low_x[:, row, :], high_x[:, row, :]
        inv = 1.0 / (1.0 + cen_x[:, row, :] - sub * p_prev)
        p, s = sup * inv, sub * inv
        fill = -s * f_prev
        inv_x[:, row, :] = inv
        s_x[:, row, :] = s
        p_x[:, row, :] = p
        f_x[:, row, :] = fill
        q_x[:, row, :] = q
        return p, fill, -q * p, e_sum + q * fill

    def y_factor(t, p_prev):
        row = pl.ds(jnp.where(first_y, t, NJ - 1 - t), 1)
        low = a_t[row, :]
        inv = 1.0 / (b_t[row, :] - low * p_prev)
        p = c_t[row, :] * inv
        inv_t[row, :] = inv
        s_t[row, :] = low * inv
        ratio_out[row, :] = p
        return p

    def halo_copy(fb):
        rows = pl.ds(pl.multiple_of(fb * S, S), S)
        return pltpu.make_async_remote_copy(
            halo_send.at[rows, :], halo_recv.at[rows, :], halo_ss.at[fb], halo_rs.at[fb],
            device_id=beside, device_id_type=MESH)

    def turn_in(fb):
        for jb in range(JB):
            in_copy(fb, jb).wait()
        views = [u_in.at[fb, jb].reshape(NI * S, L) for jb in range(JB)]

        def one(f, _):
            parts = [views[jb][pl.ds(f, NI, stride=S), :].T for jb in range(JB)]
            for jb in range(JB):
                b2[pl.ds((fb * S + f) * HW + HR + jb * L, L), :] = parts[jb]
            halo_send[pl.ds(fb * S + f, 1), :] = jnp.where(
                first_y, parts[JB - 1][L - 1:L, :], parts[0][0:1, :])
            return 0

        spelled(S, one, 0)

    def factors(n, state):
        x_state, p = state
        x_state = spelled(NI // FB, lambda r, st: x_factor(n * (NI // FB) + r, st), x_state)
        return x_state, spelled(YT, lambda r, q: y_factor(n * YT + r, q), p)

    def to_columns(fb, state):
        turn_in(fb)
        state = factors(fb - 1, state)
        halo_copy(fb).start()
        return state

    turn_in(0)
    pl.semaphore_wait(barrier, 4)
    halo_copy(0).start()

    for copy in cf_copies:
        copy.wait()
    for jb in range(JB):
        cols = slice(jb * L, (jb + 1) * L)
        d = dy[:, cols].T
        lo = sy[:, cols].T
        hi = uy[:, cols].T
        cen_t[cols, :] = 1.0 - d
        b_t[cols, :] = 1.0 + d
        lo_t[cols, :] = lo
        hi_t[cols, :] = hi
        a_t[cols, :] = jnp.where(first_y, lo, hi)
        c_t[cols, :] = jnp.where(first_y, hi, lo)

    none = jnp.zeros((JB, 1, L), f32)
    state = lax.fori_loop(1, FB, to_columns, ((none, none + 1.0, none + 1.0, none), none[0]))
    (p_last, f_last, q_all, e_sum), p_part = factors(FB - 1, state)
    for r, value in enumerate((e_sum, f_last, q_all, -p_last)):
        coef_send[:, r:r + 1, :] = value
    coef_send[:, 4:8, :] = jnp.zeros((JB, 4, L), f32)
    coef_copy = pltpu.make_async_remote_copy(
        coef_send, coef_recv, coef_ss, coef_rs, device_id=mate, device_id_type=MESH)
    ymu_copy = pltpu.make_async_remote_copy(
        ymu_send, ymu_recv, y_ss.at[2], y_rs.at[2], device_id=beside, device_id_type=MESH)

    here = my_x < 4
    g_a = b2.at[pl.ds(0, HB * NJ * PITCH), :].reshape(HB, NJ * PITCH, L)

    def paced(value, tag):
        return jnp.where(here, value, tag)

    def set_halo(fb):
        def one(f, _):
            halo = halo_recv[pl.ds(fb * S + f, 1), :]
            none = jnp.zeros_like(halo)
            b2[pl.ds((fb * S + f) * HW + HR - 1, 1), :] = jnp.where(first_y, none, halo)
            b2[pl.ds((fb * S + f) * HW + HR + NJ, 1), :] = jnp.where(first_y, halo, none)
            return 0

        spelled(S, one, 0)

    def stencil(c, h, fs, jb):
        cols = slice(jb * L, (jb + 1) * L)
        cen, lo, hi = cen_t[cols, :], lo_t[cols, :], hi_t[cols, :]
        tags = []
        for f in fs:
            at = ((c * CB + h) * S + f) * HW + HR + jb * L
            r = cen * b2[pl.ds(at, L), :] - lo * b2[pl.ds(at - 1, L), :] - hi * b2[pl.ds(at + 1, L), :]
            rt = r.T
            b1s[c][h, jb, pl.ds(f, NI, stride=PITCH), :] = rt
            tags.append(rt[0:S, :])
        return tags[0]

    def fl_copy(c):
        return pltpu.make_async_remote_copy(
            fl_send.at[c], fl_recv.at[c], fl_ss.at[c], fl_rs.at[c], device_id=mate, device_id_type=MESH)

    def part_copy(c, to, source):
        return pltpu.make_async_remote_copy(
            part_send.at[c], part_recv.at[c, source], part_ss.at[c, to], part_rs.at[c, source],
            device_id={"x": 2 * (1 - chip) + to}, device_id_type=MESH)

    mu_copy = pltpu.make_async_remote_copy(
        mu_send, mu_recv, mu_ss, mu_rs, device_id=across, device_id_type=MESH)

    def x_forward_rows(c, base, n, state):
        def row(r, state):
            i = base + r
            g, acc = state
            g = b1s[c][:, :, pl.ds(i * PITCH, S), :] * bcast_x(inv_x, i) - bcast_x(s_x, i) * g
            b3s[c][:, :, i] = g
            return g, acc + bcast_x(q_x, i) * g

        return spelled(n, row, state)

    def forward_stage(c, nxt):
        if nxt is not None:
            for h in range(CB):
                halo_copy(nxt * CB + h).wait_recv()

        def half(h, state):
            if nxt is not None:
                set_halo(nxt * CB + h)
            span = NI // CB
            n = span // (S // FP * JB)

            def part(k, carry):
                (g, acc), tags = carry
                for jb in range(JB):
                    if c is not None:
                        if nxt is not None:
                            g = paced(g, tags[0])
                        g, acc = x_forward_rows(c, h * span + (k * JB + jb) * n, n, (g, acc))
                    if nxt is not None:
                        tags = tags[1:] + (stencil(nxt, h, [FP * k + m for m in range(FP)], jb),)
                return (g, acc), tags

            return spelled(S // FP, part, (state, (jnp.zeros((S, L), f32),) * FLAG))[0]

        zeros = jnp.zeros((CB, JB, S, L), f32)
        g, acc = lax.fori_loop(0, CB, half, (zeros, zeros))
        if c is not None:
            fl_send[c, 0] = acc
            fl_send[c, 1] = g
            fl_copy(c).start()

    def pair_coefs():
        def both(row):
            mine, other = coef_send[:, row:row + 1, :], coef_recv[:, row:row + 1, :]
            return jnp.where(first_core, mine, other), jnp.where(first_core, other, mine)

        ef, el, qf, ql = both(0), both(1), both(2), both(3)
        return ef, el, qf, ql, 1.0 / (1.0 - ql[0] * ef[1])

    def own_mu():
        ef, el, qf, ql, det = pair_coefs()
        return jnp.where(first_chip, el[1] * det * ql[0] * qf[1] + ql[1], ef[0] + qf[0] * ef[1] * det * el[0])

    def up(rows):
        return jnp.broadcast_to(rows, (CB, JB, S, L))

    def pair_data(c):
        f_mine, f_other = fl_send[c, 0], fl_recv[c, 0]
        l_mine, l_other = fl_send[c, 1], fl_recv[c, 1]
        f0, f1 = jnp.where(first_core, f_mine, f_other), jnp.where(first_core, f_other, f_mine)
        l0, l1 = jnp.where(first_core, l_mine, l_other), jnp.where(first_core, l_other, l_mine)
        return f0, f1, l0, l1

    def own_weights():
        ef, el, qf, ql, det = pair_coefs()
        zero, one = jnp.zeros_like(det), jnp.ones_like(det)
        of_first = jnp.where(first_chip, jnp.where(first_core, zero, el[1] * det * ql[0]),
                             jnp.where(first_core, one, qf[0] * (1.0 + ef[1] * det * ql[0])))
        of_last = jnp.where(first_chip, jnp.where(first_core, el[1] * det, one),
                            jnp.where(first_core, qf[0] * ef[1] * det, zero))
        return of_first, of_last

    def contribute(c):
        part_send[c] = up(weights[0]) * fl_send[c, 0] + up(weights[1]) * fl_send[c, 1]
        for to in range(2):
            part_copy(c, to, core).start()

    def settle(c):
        fl_copy(c).wait_recv()
        for source in range(2):
            part_copy(c, 0, source).wait_recv()
        ef, el, qf, ql, det = pair_coefs()
        f0, f1, l0, l1 = pair_data(c)
        zero_last0 = up(det) * (l0 + up(ql[0]) * f1)
        lam_mine = jnp.where(first_chip, l1 + up(el[1]) * zero_last0,
                             f0 + up(qf[0]) * (f1 + up(ef[1]) * zero_last0))
        lam_other = part_recv[c, 0] + part_recv[c, 1]
        mu_mine, mu_other = mu_send[...], mu_recv[...]
        scale = 1.0 / (1.0 - mu_mine * mu_other)
        mid = (lam_other + mu_other[None] * lam_mine) * scale[None]
        zero = jnp.zeros_like(mid)
        prev, nxt = jnp.where(first_chip, zero, mid), jnp.where(first_chip, mid, zero)
        rest = f1 + up(qf[1]) * nxt
        last0 = up(det) * (l0 + up(el[0]) * prev + up(ql[0]) * rest)
        first1 = rest + up(ef[1]) * last0
        wprev[c] = jnp.where(first_core, prev, last0)
        wnext[c] = jnp.where(first_core, first1, nxt)

    def x_backward_rows(c, base, n, prev, w):
        def row(r, w):
            i = base + (n - 1 - r)
            w = b3s[c][:, :, i] + bcast_x(f_x, i) * prev - bcast_x(p_x, i) * w
            at = pl.ds(i * PITCH, S)
            b1s[c][:, :, at, :] = w + (w - b1s[c][:, :, at, :])
            return w

        return spelled(n, row, w)

    def backward_stage(c, prior):
        prevs = wprev[c] if c is not None else None

        def half(h, ws):
            span = NI // CB

            n = span // (S * JB)

            def part(f, carry):
                ws, tags = carry
                for jb in range(JB):
                    if c is not None:
                        if prior is not None:
                            ws = paced(ws, tags[0])
                        base = (CB - 1 - h) * span + (S * JB - 1 - f * JB - jb) * n
                        ws = x_backward_rows(c, base, n, prevs, ws)
                    if prior is not None:
                        g_ref = g_a if prior < HC else g_b
                        cols = b1s[prior][h, jb, pl.ds(f, NI, stride=PITCH), :].T
                        g_ref[(prior % HC) * CB + h, pl.ds(jb * L * PITCH + f, L, stride=PITCH), :] = cols
                        tags = tags[1:] + (cols[0:S, :],)
                return ws, tags

            return spelled(S, part, (ws, (jnp.zeros((S, L), f32),) * LAG))[0]

        start = wnext[c] if c is not None else 0
        lax.fori_loop(0, CB, half, start)

    def y_copy(half):
        rows = pl.ds(half * HB, HB)
        return pltpu.make_async_remote_copy(
            yl_send.at[rows], yl_recv.at[rows], y_ss.at[half], y_rs.at[half],
            device_id=beside, device_id_type=MESH)

    def y_edges(half):
        y_copy(half).wait_recv()
        mu_mine, mu_other = ymu_send[...], ymu_recv[...]
        scale = 1.0 / (1.0 - mu_mine * mu_other)
        rows = slice(half * HB, (half + 1) * HB)
        return (yl_recv[rows] + mu_other * yl_send[rows]) * scale

    coef_copy.start()
    forward_stage(None, 0)
    forward_stage(0, 1)
    coef_copy.wait_recv()
    mu_send[...] = jnp.broadcast_to(own_mu(), (JB, S, L))
    weights = own_weights()
    contribute(0)
    for c in range(1, CH):
        forward_stage(c, c + 1 if c + 1 < CH else None)
        contribute(c)
        if c == 1:
            mu_copy.start()

    def y_factors(first, count, p):
        def group(t, p):
            return spelled(S, lambda r, q: y_factor(first + t * S + r, q), p)

        return lax.fori_loop(0, count // S, group, p)

    p_end = y_factors(YT * FB, NJ - YT * FB, p_part)
    ymu_send[...] = jnp.broadcast_to(-p_end, (S, L))
    mu_copy.wait_recv()
    settle(0)
    backward_stage(0, None)
    ymu_copy.start()
    for c in range(1, CH):
        if c == HC + 1:
            y_eliminate(first_y, g_a, inv_t, s_t, yl_send, 0)
            y_copy(0).start()
        settle(c)
        backward_stage(c, c - 1)
    backward_stage(None, CH - 1)
    y_eliminate(first_y, g_b, inv_t, s_t, yl_send, HB)
    y_copy(1).start()
    ymu_copy.wait_recv()
    y_substitute(first_y, g_a, ratio_out, y_edges(0))
    for fb in range(HB):
        to_rows(g_a, fb, done_a)
    edge_out[...] = y_edges(1)

    ymu_copy.wait_send()
    coef_copy.wait_send()
    mu_copy.wait_send()
    for half in range(2):
        y_copy(half).wait_send()
    for fb in range(FB):
        halo_copy(fb).wait_send()
    for c in range(CH):
        fl_copy(c).wait_send()

    for c in range(CH):
        for to in range(2):
            part_copy(c, to, core).wait_send()


def finish_kernel(done_a, g_ref, edge_ref, ratio_ref, out_hbm, buf, out_sem):
    first_y = lax.axis_index("y") == 0

    def out_copy(ref, fb, jb, first):
        k = fb * JB + jb
        return pltpu.make_async_copy(
            ref.at[k], out_hbm.at[:, pl.ds((first + fb) * S, S), pl.ds(jb * L, L)],
            out_sem.at[first * JB + k])

    for fb in range(HB):
        for jb in range(JB):
            out_copy(done_a, fb, jb, 0).start()
    y_substitute(first_y, g_ref, ratio_ref, edge_ref[...])
    for fb in range(HB):
        to_rows(g_ref, fb, buf, lambda jb, fb=fb: out_copy(buf, fb, jb, HB).start())
    for fb in range(HB):
        for jb in range(JB):
            out_copy(done_a, fb, jb, 0).wait()
            out_copy(buf, fb, jb, HB).wait()


def solution(mesh):
    tile_spec = P(("batch", "x"), "y", None)
    coef_spec = P(("batch", "x"), "y")
    vmem = pl.BlockSpec(memory_space=pltpu.VMEM)
    hbm = pl.BlockSpec(memory_space=pltpu.HBM)
    V, DMA = pltpu.VMEM, pltpu.SemaphoreType.DMA
    row_x, col_t = V((JB, NI, L), f32), V((NJ, NI), f32)

    def local_step(field, *coefs):
        done, g, edge, ratio = pl.pallas_call(
            reduce_kernel,
            out_shape=(jax.ShapeDtypeStruct((HB * JB, NI, S, L), f32),
                       jax.ShapeDtypeStruct((HB, NJ * PITCH, L), f32),
                       jax.ShapeDtypeStruct((HB, S, L), f32),
                       jax.ShapeDtypeStruct((NJ, L), f32)),
            in_specs=[hbm] * 7,
            out_specs=(vmem, vmem, vmem, vmem),
            scratch_shapes=[
                V((FB, JB, NI, S, L), f32), [V((CB, JB, NI * PITCH, L), f32)] * CH, V((NF * HW, L), f32), [V((CB, JB, NI, S, L), f32)] * CH,
                V((NF, L), f32), V((NF, L), f32),
                row_x, row_x, row_x, row_x, row_x, row_x, row_x, row_x,
                V((NI, NJ), f32), V((NI, NJ), f32), V((NI, NJ), f32),
                col_t, col_t, col_t, col_t, col_t, col_t, col_t, col_t,
                V((JB, S, L), f32), V((JB, S, L), f32), V((JB, S, L), f32), V((JB, S, L), f32),
                V((CH, 2, CB, JB, S, L), f32), V((CH, 2, CB, JB, S, L), f32),
                V((CH, CB, JB, S, L), f32), V((CH, 2, CB, JB, S, L), f32),
                V((CH, CB, JB, S, L), f32), V((CH, CB, JB, S, L), f32),
                V((FB, S, L), f32), V((FB, S, L), f32), V((S, L), f32), V((S, L), f32),
                DMA((9,)), DMA((FB * JB,)), DMA((FB,)), DMA((FB,)), DMA, DMA, DMA, DMA,
                DMA((CH,)), DMA((CH,)), DMA((CH, 2)), DMA((CH, 2)), DMA((3,)), DMA((3,)),
            ],
            compiler_params=pltpu.CompilerParams(
                collective_id=0, has_side_effects=True, vmem_limit_bytes=RL),
            name="reduce",
        )(*(pltpu.with_memory_space_constraint(x, pltpu.HBM) for x in (jnp.swapaxes(field, 1, 2), *coefs)))
        out = pl.pallas_call(
            finish_kernel,
            out_shape=jax.ShapeDtypeStruct((NI, NF, NJ), f32),
            in_specs=[vmem] * 4,
            out_specs=hbm,
            scratch_shapes=[V((HB * JB, NI, S, L), f32), DMA((FB * JB,))],
            compiler_params=pltpu.CompilerParams(vmem_limit_bytes=FL << 20),
            name="finish",
        )(done, g, edge, ratio)
        return jnp.swapaxes(out, 1, 2)

    return jax.shard_map(local_step, mesh=mesh, in_specs=(tile_spec,) + (coef_spec,) * 6,
                         out_specs=tile_spec, check_vma=False)
```
